128 devices in a mesh: node: 16 (over y, x), grp: 8 (over z, core).
Axes of the slice: x: 4, y: 4, z: 4, core: 2. Of those that a mesh axis runs over, the one named last changes fastest.
Arguments:
- tokens: bfloat16 [49152, 1792], P(('node', 'grp')), may hold values from -6 to 6
- cotangent: bfloat16 [49152, 1792], P(('node', 'grp')), may hold values from -6 to 6
- gate_weight: bfloat16 [1792, 1024], P('node'), may hold values from -0.125 to 0.125
- up_weight: bfloat16 [1792, 1024], P('node'), may hold values from -0.125 to 0.125
- down_weight_t: bfloat16 [1792, 1024], P('node'), may hold values from -0.125 to 0.125
- error_memory: bfloat16 [8, 1792, 3072], P('grp', 'node'), may hold values from -4 to 4
- q_init: float32 [3, 1024, 32], replicated, may hold values from -6 to 6
Outputs:
- token_grad: bfloat16 [49152, 1792], P(('node', 'grp'))
- new_error: bfloat16 [8, 1792, 3072], P('grp', 'node')
- p_hat: float32 [3, 1792, 32], P(None, 'node')
- q_new: float32 [3, 1024, 32], replicated
The draws below stay inside these ranges and needn't reach their ends.
All inputs are finite; a program needn't handle non-finite values.
Results may differ from the reference program's by a relative error of at most 0.012.
Values may be sent and summed in bfloat16 or wider, within the bound.
No kernel may reach another device: no remote copies, remote signals or barrier semaphores. Data moves between devices by JAX's collectives and lax.ppermute only.
A program may use at most 192 MiB of HBM per device.

```python
import math
import jax
import jax.numpy as jnp
from jax import lax

D = 1792
H = 1024
R = 32
TOK_DEV = 384
TOKENS = 49152
N_NODE = 16
N_GRP = 8


def block_levels(rng, dims, cuts, least, high):
    factor_of, own = 1.0, jax.random.fold_in(rng, 6)
    for position, parts in cuts:
        heights = jnp.exp(jax.random.uniform(jax.random.fold_in(own, position), (parts,), jnp.float32, least / len(cuts), high / len(cuts)))
        factor_of = factor_of * jnp.repeat(heights, dims[position] // parts).reshape([-1 if axis == position else 1 for axis in range(len(dims))])
    return factor_of


def normal_values(own_key, extent, scale, bound, pieces=(), kind=jnp.bfloat16):
    entries = jax.random.normal(own_key, extent, jnp.float32) * scale
    if len(pieces) > 0:
        entries = block_levels(own_key, extent, pieces, -0.22, 0.18) * entries
    return jnp.clip(entries, min=-bound, max=bound).astype(kind)


def setup_inputs(seed: int = 0) -> dict:
    arg_keys = jax.random.split(jax.random.key(seed), 8)
    return {
        "tokens": normal_values(arg_keys[0], (TOKENS, D), 1.0, 6.0, ((0, 128),)),
        "cotangent": normal_values(arg_keys[1], (TOKENS, D), 1.0, 6.0, ((0, 128),)),
        "gate_weight": normal_values(arg_keys[2], (D, H), D ** -0.5, 0.125, ((0, 16),)),
        "up_weight": normal_values(arg_keys[3], (D, H), D ** -0.5, 0.125, ((0, 16),)),
        "down_weight_t": normal_values(arg_keys[4], (D, H), D ** -0.5, 0.125, ((0, 16),)),
        "error_memory": normal_values(arg_keys[5], (N_GRP, D, 3 * H), 0.5, 4.0, ((0, 8), (1, 16))),
        "q_init": normal_values(arg_keys[6], (3, H, R), 1.0, 6.0, (), jnp.float32),
    }


def gelu_parts(value):
    coeff = math.sqrt(2.0 / math.pi)
    inner = coeff * (value + 0.044715 * value * value * value)
    tanh_value = jnp.tanh(inner)
    activation = 0.5 * value * (1.0 + tanh_value)
    slope = 0.5 * (1.0 + tanh_value) + 0.5 * value * (1.0 - tanh_value * tanh_value) * coeff * (1.0 + 3.0 * 0.044715 * value * value)
    return (activation, slope)

def arrange(values):
    return values.reshape(N_NODE, N_GRP, TOK_DEV, -1).transpose(1, 0, 2, 3).reshape(N_GRP, N_NODE * TOK_DEV, -1)

def group_grad(items):
    token_rows, cot_rows, gate_up, hidden = items
    left_part = jnp.dot(token_rows.T.astype(jnp.float32), gate_up.astype(jnp.float32), preferred_element_type=jnp.float32)
    right_part = jnp.dot(cot_rows.T.astype(jnp.float32), hidden.astype(jnp.float32), preferred_element_type=jnp.float32)
    return jnp.concatenate([left_part, right_part], axis=1)

def reference(tokens, cotangent, gate_weight, up_weight, down_weight_t, error_memory, q_init):
    hidden_units = gate_weight.shape[1]
    gate_pre = jnp.dot(tokens.astype(jnp.float32), gate_weight.astype(jnp.float32), preferred_element_type=jnp.float32)
    up_pre = jnp.dot(tokens.astype(jnp.float32), up_weight.astype(jnp.float32), preferred_element_type=jnp.float32)
    activation, slope = gelu_parts(gate_pre)
    hidden = (activation * up_pre).astype(jnp.bfloat16)
    back_hidden = jnp.dot(cotangent.astype(jnp.float32), down_weight_t.astype(jnp.float32), preferred_element_type=jnp.float32)
    grad_up = (back_hidden * activation).astype(jnp.bfloat16)
    grad_gate = (back_hidden * up_pre * slope).astype(jnp.bfloat16)
    token_grad = (jnp.dot(grad_gate.astype(jnp.float32), gate_weight.T.astype(jnp.float32), preferred_element_type=jnp.float32) + jnp.dot(grad_up.astype(jnp.float32), up_weight.T.astype(jnp.float32), preferred_element_type=jnp.float32)).astype(jnp.bfloat16)
    gate_up = jnp.concatenate([grad_gate, grad_up], axis=1)
    grads = lax.map(group_grad, (arrange(tokens), arrange(cotangent), arrange(gate_up), arrange(hidden)))
    grad_scale = 1.0 / math.sqrt(TOK_DEV * N_NODE)
    merged = grads * grad_scale + error_memory.astype(jnp.float32)
    hats = []
    rights = []
    errors = []
    for m in range(3):
        matrix_block = merged[:, :, m * hidden_units:(m + 1) * hidden_units]
        power = jnp.einsum('kdh,hr->dr', matrix_block, q_init[m], precision=lax.Precision.HIGHEST) / N_GRP
        gram_matrix = jnp.dot(power.T, power, precision=lax.Precision.HIGHEST)
        factor = jnp.linalg.cholesky(gram_matrix)
        left_hat = jax.scipy.linalg.solve_triangular(factor, power.T, lower=True).T
        right_new = jnp.einsum('kdh,dr->hr', matrix_block, left_hat, precision=lax.Precision.HIGHEST) / N_GRP
        rebuilt = jnp.dot(left_hat, right_new.T, precision=lax.Precision.HIGHEST)
        errors.append(matrix_block - rebuilt[None])
        hats.append(left_hat)
        rights.append(right_new)
    new_error = jnp.concatenate(errors, axis=2).astype(jnp.bfloat16)
    return (token_grad, new_error, jnp.stack(hats), jnp.stack(rights))
```

```python
import math

import jax
import jax.numpy as jnp
from jax import lax
from jax.experimental import pallas as pl
from jax.experimental.pallas import tpu as pltpu
from jax.sharding import Mesh
from jax.sharding import PartitionSpec as P

Y, X, Z, C = "node_0", "node_1", "grp_0", "grp_1"
NODE = (Y, X)
GRP = (Z, C)
NODE_GRP = (Y, X, Z, C)
BF = jnp.bfloat16
F32 = jnp.float32


def shift(value, axis, by):
    size = lax.axis_size(axis)
    return lax.ppermute(value, axis, [(i, (i + by) % size) for i in range(size)])


def halves(value):
    at = value.shape[-1] // 2
    return value[..., :at], value[..., at:]


def ring_gather(block, axis):
    low, high = halves(block)
    from_left, from_right = shift(block, axis, 1), shift(block, axis, -1)
    far_low = shift(halves(from_left)[0], axis, 1)
    far_high = shift(halves(from_right)[1], axis, -1)
    far = jnp.concatenate([far_low, far_high], axis=-1)
    return [block, from_right, far, from_left]


def ring_scatter(part_of, axis):
    far_low, far_high = halves(part_of(2, ()))
    to_right, to_left = shift(far_low, axis, 1), shift(far_high, axis, -1)
    right = part_of(1, ((0, to_right),))
    left = part_of(3, ((1, to_left),))
    return part_of(0, ((None, shift(right, axis, 1)), (None, shift(left, axis, -1))))


def with_terms(value, terms):
    for side, term in terms:
        if side is None:
            value = value + term.astype(F32)
        else:
            low, high = halves(value)
            if side == 0:
                low = low + term.astype(F32)
            else:
                high = high + term.astype(F32)
            value = jnp.concatenate([low, high], axis=-1)
    return value


def exchange(tiles, axis):
    return lax.all_to_all(tiles, axis, split_axis=0, concat_axis=0, tiled=True)


def from_everyone(shard, axis):
    return exchange(jnp.broadcast_to(shard, (lax.axis_size(axis), *shard.shape)), axis)


def gelu_parts(value):
    coeff = math.sqrt(2.0 / math.pi)
    inner = coeff * (value + 0.044715 * value * value * value)
    tanh_value = jnp.tanh(inner)
    activation = 0.5 * value * (1.0 + tanh_value)
    slope = 0.5 * (1.0 + tanh_value) + 0.5 * value * (1.0 - tanh_value * tanh_value) * coeff * (
        1.0 + 3.0 * 0.044715 * value * value
    )
    return (activation, slope)


def dot(a, b, ca=1, cb=0, precision=None):
    return lax.dot_general(
        a, b, (((ca,), (cb,)), ((), ())), precision=precision, preferred_element_type=F32
    )


def inverse_factor_body(gram_ref, out_ref):
    r = gram_ref.shape[-1]
    rows = lax.broadcasted_iota(jnp.int32, (3, r, 2 * r), 1)
    cols = lax.broadcasted_iota(jnp.int32, (3, r, 2 * r), 2)
    both = jnp.concatenate([gram_ref[...], jnp.zeros((3, r, r), F32)], axis=2)
    both = both + jnp.where(cols == rows + r, 1.0, 0.0)
    scale = jnp.zeros((3, r, 1), F32)
    for j in range(r):
        column = both[:, :, j : j + 1]
        pivot = both[:, j : j + 1, j : j + 1]
        row = both[:, j : j + 1, :]
        scale = jnp.where(rows[:, :, :1] == j, 1.0 / jnp.sqrt(pivot), scale)
        factor = jnp.where(rows[:, :, :1] > j, column / pivot, 0.0)
        both = both - factor * row
    out_ref[...] = both[:, :, r:] * scale


def inverse_factor(gram):
    return pl.pallas_call(
        inverse_factor_body, out_shape=jax.ShapeDtypeStruct(gram.shape, F32)
    )(gram)


def rolled_rows(tokens, first, second, swap):
    blocks = tokens.T.reshape(4, 4, -1, tokens.shape[0])
    blocks = lax.dynamic_slice_in_dim(jnp.concatenate([blocks, blocks], 0), first, 4, 0)
    blocks = lax.dynamic_slice_in_dim(jnp.concatenate([blocks, blocks], 1), second, 4, 1)
    if swap:
        blocks = jnp.swapaxes(blocks, 0, 1)
    return blocks.reshape(4, -1, tokens.shape[0])


def forward(tokens, cotangent, gate, up, down):
    gate_pre = dot(tokens, gate)
    up_pre = dot(tokens, up)
    activation, slope = gelu_parts(gate_pre)
    hidden = (activation * up_pre).astype(BF)
    back_hidden = dot(cotangent, down)
    grad_up = (back_hidden * activation).astype(BF)
    grad_gate = (back_hidden * up_pre * slope).astype(BF)
    return grad_gate, grad_up, hidden


def on_device(tokens, cotangent, gate_weight, up_weight, down_weight_t, error_memory, q_init):
    yi, xi, core = lax.axis_index(Y), lax.axis_index(X), lax.axis_index(C)
    rows, units = gate_weight.shape
    group_count = lax.axis_size(GRP)
    half, rank = units // 2, q_init.shape[-1]
    width = tokens.shape[1]
    grad_scale = 1.0 / math.sqrt(tokens.shape[0] * lax.axis_size(NODE))

    def mine(value, dim, flip=0):
        at = (core + flip) % 2 if flip else core
        return lax.dynamic_slice_in_dim(value, at * half, half, dim)

    quarter = half // 2
    own = [mine(w, 1) for w in (gate_weight, up_weight, down_weight_t)]
    first = jnp.concatenate([w[:, :quarter] for w in own], axis=1)
    second = jnp.concatenate([w[:, quarter:] for w in own], axis=1)
    near_x, near_y = ring_gather(first, X), ring_gather(second, Y)
    plane_x = ring_gather(jnp.stack(near_x), Y)
    plane_y = ring_gather(jnp.stack(near_y), X)
    full = jnp.zeros((2, 4, 4, rows, 3 * quarter), BF)
    for a in range(4):
        for b in range(4):
            ya, xb = (yi + a) % 4, (xi + b) % 4
            full = lax.dynamic_update_slice(full, plane_x[a][b][None, None, None], (0, ya, xb, 0, 0))
            full = lax.dynamic_update_slice(full, plane_y[b][a][None, None, None], (1, ya, xb, 0, 0))
    full = full.reshape(2, width, 3 * quarter)
    gate, up, down = (
        jnp.concatenate([full[0][:, at : at + quarter], full[1][:, at : at + quarter]], axis=1)
        for at in (0, quarter, 2 * quarter)
    )

    other_tokens, other_cot = shift(tokens, C, 1), shift(cotangent, C, 1)
    error = error_memory[0]
    error_3 = error.reshape(rows, 3, units)
    error_sum = mine(error_3, 2).astype(F32) + shift(mine(error_3, 2, 1), C, 1).astype(F32)
    q_mine = mine(q_init, 1)

    pairs = ((tokens, cotangent), (other_tokens, other_cot))
    grads = [forward(t, c, gate, up, down) for t, c in pairs]

    summed = []
    for m, ((t, c), (g_gate, g_up, hid)) in enumerate(zip(pairs, grads)):
        by_x = m == 0
        t_rows, c_rows = (rolled_rows(v, yi, xi, by_x) for v in (t, c))
        gate_up = jnp.concatenate([g_gate, g_up], axis=1)

        def product(at, terms, t_rows=t_rows, c_rows=c_rows, gate_up=gate_up, hid=hid):
            value = jnp.concatenate([dot(t_rows[at], gate_up), dot(c_rows[at], hid)], axis=1)
            return with_terms(value, terms).astype(BF)

        line = ring_scatter(product, X if by_x else Y).reshape(4, rows, -1)

        def piece(at, terms, line=line):
            return with_terms(line[at].astype(F32), terms).astype(BF)

        summed.append(ring_scatter(piece, Y if by_x else X))
    kept, partner = summed[0], shift(summed[1], C, 1)
    kept, partner = (v.reshape(rows, 3, half) for v in (kept, partner))
    low = jnp.where(core == 0, kept, partner)
    high = jnp.where(core == 0, partner, kept)
    grad_rows = jnp.concatenate([low, high], axis=2).reshape(rows, 3 * units)

    sides = [dot(g, gate, 1, 1) + dot(u, up, 1, 1) for g, u, _ in grads]
    token_grad = (sides[0] + shift(sides[1].astype(BF), C, 1).astype(F32)).astype(BF)

    both_t = jnp.concatenate([tokens, other_tokens], axis=0)
    both_c = jnp.concatenate([cotangent, other_cot], axis=0)
    g_gate, g_up, hid = (jnp.concatenate([a, b], axis=0) for a, b in zip(*grads))
    q_low = q_mine.astype(BF)
    projected = jnp.concatenate([dot(g_gate, q_low[0]), dot(g_up, q_low[1])], axis=1).astype(BF)
    projected_hid = dot(hid, q_low[2]).astype(BF)
    terms = jnp.concatenate([dot(both_t, projected, 0, 0), dot(both_c, projected_hid, 0, 0)], axis=1)
    error_part = jnp.concatenate([dot(error_sum[:, m], q_mine[m]) for m in range(3)], axis=1)
    row_first = (yi * 4 + xi) * rows
    placed = lax.dynamic_update_slice_in_dim(jnp.zeros_like(terms), error_part, row_first, 0)
    terms = (terms * grad_scale + placed) * (1.0 / group_count)
    mine_p = exchange(terms.astype(BF).reshape(group_count, -1, 3 * rank), GRP).astype(F32).sum(0)
    mine_p = from_everyone(mine_p.astype(BF), NODE).astype(F32).sum(0)
    power = from_everyone(mine_p.astype(BF), GRP).reshape(width, 3 * rank)

    seen = dot(both_t, power[:, : 2 * rank]).astype(BF)
    seen_hid = dot(both_c, power[:, 2 * rank :]).astype(BF)
    right = jnp.concatenate(
        [
            dot(seen[:, :rank], g_gate, 0, 0),
            dot(seen[:, rank:], g_up, 0, 0),
            dot(seen_hid, hid, 0, 0),
        ],
        axis=0,
    )
    power_rows = lax.dynamic_slice_in_dim(power, row_first, rows, 0).astype(F32)
    power_3 = power_rows.reshape(rows, 3, rank)
    error_right = jnp.concatenate(
        [dot(power_3[:, m], error_sum[:, m], 0, 0) for m in range(3)], axis=0
    )
    right = (right * grad_scale + error_right) * (1.0 / group_count)
    tiles = jnp.swapaxes(right.astype(BF).reshape(3 * rank, 4, -1), 0, 1)
    mine_b = exchange(tiles, Z).astype(F32).sum(0)
    mine_b = from_everyone(mine_b.astype(BF), NODE).astype(F32).sum(0)
    everyone = from_everyone(mine_b.astype(BF), (C, Z))
    right = jnp.swapaxes(everyone, 0, 1).reshape(3, rank, units).astype(F32)

    power_all = power.astype(F32).reshape(width, 3, rank)
    high_p = lax.Precision.HIGHEST
    gram = jnp.stack([dot(power_all[:, m], power_all[:, m], 0, 0, high_p) for m in range(3)])
    inverse = inverse_factor(gram)
    hats = jnp.stack([dot(power_3[:, m], inverse[m], 1, 1, high_p) for m in range(3)])
    q_t = [dot(inverse[m], right[m], 1, 0, high_p) for m in range(3)]
    rebuilt = jnp.concatenate([dot(hats[m], q_t[m]) for m in range(3)], axis=1)
    merged = grad_rows.astype(F32) * grad_scale + error.astype(F32)
    new_error = (merged - rebuilt).astype(BF)[None]
    q_new = jnp.stack([q.T for q in q_t])
    return (token_grad, new_error, hats, q_new)


def solution(mesh):
    finer = Mesh(mesh.devices.reshape(4, 4, 4, 2), NODE_GRP)
    placed = (
        P(NODE_GRP, None),
        P(NODE_GRP, None),
        P(NODE, None),
        P(NODE, None),
        P(NODE, None),
        P(GRP, NODE, None),
        P(),
    )
    return jax.shard_map(
        on_device,
        mesh=finer,
        in_specs=placed,
        out_specs=(P(NODE_GRP, None), P(GRP, NODE, None), P(None, NODE, None), P()),
        check_vma=False,
    )
```

```python
import functools
import math

import jax
import jax.numpy as jnp
from jax import lax
from jax.experimental import pallas as pl
from jax.experimental.pallas import tpu as pltpu
from jax.sharding import Mesh
from jax.sharding import PartitionSpec as P

Y, X, Z, C = "node_0", "node_1", "grp_0", "grp_1"
NODE = (Y, X)
GRP = (Z, C)
NODE_GRP = (Y, X, Z, C)
BF = jnp.bfloat16
F32 = jnp.float32
HIGH = lax.Precision.HIGHEST


def neighbour(value, stage, by):
    pairs = []
    for device in range(128):
        y, x, z, c = device // 32, device // 8 % 4, device // 2 % 4, device % 2
        if (c == 0) == (stage == 0):
            to = (y, (x + by) % 4, z, c)
        else:
            to = ((y + by) % 4, x, z, c)
        pairs.append((device, to[0] * 32 + to[1] * 8 + to[2] * 2 + to[3]))
    return lax.ppermute(value, NODE_GRP, pairs)


def other_core(value):
    return lax.ppermute(value, C, [(0, 1), (1, 0)])


def exchange(tiles, axis):
    return lax.all_to_all(tiles, axis, split_axis=0, concat_axis=0, tiled=True)


def dot(a, b, ca=1, cb=0, precision=None):
    return lax.dot_general(
        a, b, (((ca,), (cb,)), ((), ())), precision=precision, preferred_element_type=F32
    )


def call(body, out, grid=None, ins=None, outs=None, flops=0, scratch=(), vmem=24):
    params = {}
    if grid is not None:
        params.update(grid=grid, in_specs=ins, out_specs=outs)
    elif ins is not None:
        params.update(in_specs=ins)
    if flops:
        params["cost_estimate"] = pl.CostEstimate(
            flops=flops, bytes_accessed=1 << 20, transcendentals=0
        )
    return pl.pallas_call(
        body,
        out_shape=out,
        scratch_shapes=scratch,
        compiler_params=pltpu.CompilerParams(vmem_limit_bytes=vmem << 20),
        **params,
    )


SCALAR = pl.BlockSpec(memory_space=pltpu.SMEM)
WHOLE = pl.BlockSpec(memory_space=pltpu.VMEM)


def struct(shape, kind=BF):
    return jax.ShapeDtypeStruct(shape, kind)


def gelu_parts(value):
    coeff = math.sqrt(2.0 / math.pi)
    inner = coeff * (value + 0.044715 * value * value * value)
    tanh_value = jnp.tanh(inner)
    activation = 0.5 * value * (1.0 + tanh_value)
    slope = 0.5 * (1.0 + tanh_value) + 0.5 * value * (1.0 - tanh_value * tanh_value) * coeff * (
        1.0 + 3.0 * 0.044715 * value * value
    )
    return (activation, slope)


def roll_body(order_ref, own_ref, other_ref, out_ref, scratch):
    tok, rows = own_ref.shape[0], out_ref.shape[1]
    scratch[:, :tok] = own_ref[...].T
    scratch[:, tok:] = other_ref[...].T
    for s in range(out_ref.shape[0]):
        out_ref[s] = scratch[pl.ds(pl.multiple_of(order_ref[s] * rows, 16), rows), :]


def rolled(order, own, other, rows):
    tok, width = own.shape
    return call(
        roll_body,
        struct((width // rows, rows, 2 * tok)),
        ins=[SCALAR, WHOLE, WHOLE],
        scratch=[pltpu.VMEM((width, 2 * tok), BF)],
        vmem=16,
    )(order, own, other).reshape(4, 4, rows, 2 * tok)


def pair(ref, a, b):
    value = ref[a, 2 * b : 2 * b + 2]
    return value.reshape(-1, value.shape[-1])


def ahead_body(slots, t_ref, c_ref, *refs):
    out_ref = refs[-1]
    units = out_ref.shape[-1] // 3
    gate_up, back = 0.0, 0.0
    if len(refs) > len(slots) + 1:
        gate_up, back = refs[-2][:, : 2 * units], refs[-2][:, 2 * units :]
    for (a, b), piece in zip(slots, refs):
        gate_up = gate_up + dot(pair(t_ref, a, b), piece[:, : 2 * units], 0, 0)
        back = back + dot(pair(c_ref, a, b), piece[:, 2 * units :], 0, 0)
    out_ref[:, : 2 * units] = gate_up
    out_ref[:, 2 * units :] = back


def ahead(slots, t_roll, c_roll, pieces, partial=None):
    _, _, rows, both = t_roll.shape
    tok, wide = both // 2, pieces[0].shape[1]
    roll = pl.BlockSpec((4, 4, rows, tok), lambda k: (0, 0, 0, k))
    block = pl.BlockSpec((tok, wide), lambda k: (k, 0))
    ins = [roll, roll] + [pl.BlockSpec((2 * rows, wide), lambda k: (0, 0))] * len(pieces)
    more = () if partial is None else (partial,)
    return call(
        functools.partial(ahead_body, slots),
        struct((both, wide), F32),
        grid=(2,),
        ins=ins + [block] * len(more),
        outs=block,
        flops=2 * both * wide * 2 * rows * len(pieces),
        vmem=28,
    )(t_roll, c_roll, *pieces, *more)


def weight_part(t_ref, c_ref, grads):
    units = grads.shape[1] // 3
    t, c = (ref[...].reshape(-1, ref.shape[-1]) for ref in (t_ref, c_ref))
    return jnp.concatenate([dot(t, grads[:, : 2 * units]), dot(c, grads[:, 2 * units :])], axis=1)


def late_body(
    scale, groups, part_ref, t_ref, c_ref, low, high, q_ref, t_far, c_far, t_own, t_other,
    c_own, c_other, placed_ref, grads_ref, far_own, far_other, power_ref, total
):
    units = grads_ref.shape[-1] // 3
    gate_up, back = part_ref[:, : 2 * units], part_ref[:, 2 * units :]
    for b, piece in enumerate((low, high)):
        gate_up = gate_up + dot(pair(t_ref, 0, b), piece[:, : 2 * units], 0, 0)
        back = back + dot(pair(c_ref, 0, b), piece[:, 2 * units :], 0, 0)
    up_pre = gate_up[:, units:]
    activation, slope = gelu_parts(gate_up[:, :units])
    parts = (back * up_pre * slope, back * activation, activation * up_pre)
    parts = [part.astype(BF) for part in parts]
    for m, part in enumerate(parts):
        grads_ref[:, m * units : (m + 1) * units] = part
    far = weight_part(t_far, c_far, grads_ref).astype(BF)
    first = jnp.concatenate([dot(q_ref[m], parts[m], 1, 1) for m in range(2)], axis=0).astype(BF)
    second = dot(q_ref[2], parts[2], 1, 1).astype(BF)
    split = first.shape[0]

    def finish(t, c, out, last):
        out[...] = far
        top, bottom = dot(first, t[...]), dot(second, c[...])
        if not last:
            total[:split], total[split:] = top, bottom
        else:
            top, bottom = top + total[:split], bottom + total[split:]
            value = jnp.concatenate([top, bottom], axis=0)
            value = (value * scale + placed_ref[...]) * (1.0 / groups)
            step = value.shape[0] // groups
            for i in range(groups):
                power_ref[i] = value[i * step : (i + 1) * step].astype(BF)

    pl.when(pl.program_id(0) == 0)(lambda: finish(t_own, c_own, far_own, False))
    pl.when(pl.program_id(0) == 1)(lambda: finish(t_other, c_other, far_other, True))


def near_body(t_one, c_one, t_three, c_three, grads_ref, *outs):
    one = weight_part(t_one, c_one, grads_ref).astype(BF)
    three = weight_part(t_three, c_three, grads_ref).astype(BF)
    for k in range(2):

        def put(k=k):
            outs[k][...] = one
            outs[2 + k][...] = three

        pl.when(pl.program_id(0) == k)(put)


def home_body(t_ref, c_ref, grads_ref, right_own, right_other, left_own, left_other, *outs):
    value = weight_part(t_ref, c_ref, grads_ref)
    rows = outs[0].shape[0]

    def put(k, a, b):
        total = (value + a[...].astype(F32) + b[...].astype(F32)).astype(BF)
        for i in range(4):
            outs[4 * k + i][...] = total[i * rows : (i + 1) * rows]

    pl.when(pl.program_id(0) == 0)(lambda: put(0, right_own, left_own))
    pl.when(pl.program_id(0) == 1)(lambda: put(1, right_other, left_other))


def spread_body(in_ref, out_ref):
    total = in_ref[0].astype(F32)
    for i in range(1, in_ref.shape[0]):
        total = total + in_ref[i].astype(F32)
    total = total.astype(BF)
    for i in range(out_ref.shape[0]):
        out_ref[i] = total


def spread(tiles, count):
    return call(spread_body, struct((count, *tiles.shape[1:])), vmem=8)(tiles)


def stacked(p_ref):
    return jnp.concatenate([p_ref[i].astype(F32) for i in range(p_ref.shape[0])], axis=0)


def right_body(
    scale, groups, p_ref, t_own, t_other, c_own, c_other, y_ref, e_ref, pick_ref, out_ref
):
    power = stacked(p_ref).astype(BF)
    rank = power.shape[0] // 3
    units, tok = y_ref.shape[1] // 3, t_own.shape[0]
    rows = dot(power, pick_ref[...]).astype(BF)
    values = [0.0, 0.0, 0.0]
    for k, (t, c) in enumerate(((t_own, c_own), (t_other, c_other))):
        seen = dot(power[: 2 * rank], t[...], 1, 1).astype(BF)
        lhs = (seen[:rank], seen[rank:], dot(power[2 * rank :], c[...], 1, 1).astype(BF))
        y = y_ref[k * tok : (k + 1) * tok]
        values = [v + dot(lhs[m], y[:, m * units : (m + 1) * units]) for m, v in enumerate(values)]
    for m in range(3):
        value = values[m] * scale
        value = value + dot(rows[m * rank : (m + 1) * rank], e_ref[:, m * units : (m + 1) * units])
        value = (value * (1.0 / groups)).astype(BF)
        step = units // 4
        for i in range(4):
            out_ref[i, m * rank : (m + 1) * rank] = value[:, i * step : (i + 1) * step]


def factor_body(p_ref, pick_ref, inverse_ref, hats_ref):
    power = stacked(p_ref)
    r = power.shape[0] // 3
    low = power.astype(BF)
    gram = jnp.stack(
        [dot(low[m * r : (m + 1) * r], low[m * r : (m + 1) * r], 1, 1) for m in range(3)]
    )
    rows = lax.broadcasted_iota(jnp.int32, (3, r, 2 * r), 1)
    cols = lax.broadcasted_iota(jnp.int32, (3, r, 2 * r), 2)
    both = jnp.concatenate([gram, jnp.zeros((3, r, r), F32)], axis=2)
    both = both + jnp.where(cols == rows + r, 1.0, 0.0)
    for j in range(r):
        column = jnp.where(rows[:, :, :1] > j, both[:, :, j : j + 1], 0.0)
        row = both[:, j : j + 1, :] / both[:, j : j + 1, j : j + 1]
        both = both - column * row
    diagonal = jnp.sum(jnp.where(cols == rows, both, 0.0), axis=2, keepdims=True)
    inverse = both[:, :, r:] * (1.0 / jnp.sqrt(diagonal))
    inverse_ref[...] = inverse
    mine = dot(low, pick_ref[...])
    for m in range(3):
        hats_ref[m] = dot(inverse[m], mine[m * r : (m + 1) * r], 1, 0, HIGH)


def final_body(scale, core_ref, b_ref, inverse_ref, hats_ref, kept_ref, sent_ref, e_ref, err_ref, q_ref):
    r = inverse_ref.shape[1]
    units = q_ref.shape[2]
    half = units // 2
    core = core_ref[0]
    for m in range(3):
        right = jnp.concatenate(
            [b_ref[i, m * r : (m + 1) * r].astype(F32) for i in range(b_ref.shape[0])], axis=1
        )
        q_t = dot(inverse_ref[m], right, 1, 0, HIGH)
        q_ref[m] = q_t
        rebuilt = dot(hats_ref[m].astype(BF), q_t.astype(BF), 0, 0)
        kept = kept_ref[:, m * half : (m + 1) * half].astype(F32)
        sent = sent_ref[:, m * half : (m + 1) * half].astype(F32)
        for side in range(2):
            at = slice(m * units + side * half, m * units + (side + 1) * half)
            grad = jnp.where(core == side, kept, sent)
            value = grad * scale + e_ref[:, at].astype(F32)
            err_ref[0, :, at] = (value - rebuilt[:, side * half : (side + 1) * half]).astype(BF)


def token_body(order_ref, y_ref, *refs):
    own_ref, other_ref = refs[-2:]
    rows, tok = own_ref.shape[1:]
    wide = y_ref.shape[1] // 3 * 2
    for s in range(own_ref.shape[0]):
        w = refs[s // 2][s % 2 * rows : (s % 2 + 1) * rows, :wide]
        value = dot(w, y_ref[:, :wide], 1, 1).astype(BF)
        own_ref[order_ref[s]] = value[:, :tok]
        other_ref[order_ref[s]] = value[:, tok:]


def turn_body(a_ref, b_ref, out_ref):
    value = a_ref[...].astype(F32) + b_ref[...].astype(F32)
    out_ref[...] = value.T.astype(BF)


def on_device(tokens, cotangent, gate_weight, up_weight, down_weight_t, error_memory, q_init):
    yi, xi, core = lax.axis_index(Y), lax.axis_index(X), lax.axis_index(C)
    rows, units = gate_weight.shape
    node_count, groups = lax.axis_size(NODE), lax.axis_size(GRP)
    half, rank = units // 2, q_init.shape[-1]
    tok, width = tokens.shape
    grad_scale = 1.0 / math.sqrt(tok * node_count)

    def part(value, which, dim):
        return lax.dynamic_slice_in_dim(value, which * half, half, dim)

    def first(value, by):
        return neighbour(value, 0, by)

    def second(value, by):
        return neighbour(value, 1, by)

    weights = (gate_weight, up_weight, down_weight_t)
    own = jnp.concatenate([part(w, core, 1) for w in weights], axis=1)
    from_left, from_right = first(own, 1), first(own, -1)
    at = rows // 32 * 16
    far_low, far_high = first(from_left[:at], 1), first(from_right[at:], -1)
    low = jnp.concatenate([own, from_right], axis=0)
    left_low, right_low = second(low, 1), second(low, -1)
    high = jnp.concatenate([far_low, far_high, from_left], axis=0)
    left_high, right_high = second(high, 1), second(high, -1)
    over_low, over_high = second(left_low, 1), second(right_high, -1)

    over, along = jnp.arange(4)[:, None], jnp.arange(4)[None, :]
    ys = jnp.where(core == 0, yi + over, yi + along) % 4
    xs = jnp.where(core == 0, xi + along, xi + over) % 4
    order = (ys * 4 + xs).reshape(-1).astype(jnp.int32)

    other_t, other_c = other_core(tokens), other_core(cotangent)
    error = error_memory[0]
    error_3 = error.reshape(rows, 3, units)
    error_sum = part(error_3, core, 2).astype(F32) + other_core(part(error_3, 1 - core, 2)).astype(F32)
    error_sum = error_sum.reshape(rows, 3 * half)
    q_rows = jnp.swapaxes(part(q_init, core, 1), 1, 2)
    t_roll, c_roll = rolled(order, tokens, other_t, rows), rolled(order, cotangent, other_c, rows)
    row_first = (yi * 4 + xi) * rows
    error_part = jnp.concatenate(
        [dot(q_rows[m], error_sum[:, m * half : (m + 1) * half], 1, 1) for m in range(3)], axis=0
    )
    placed = lax.dynamic_update_slice_in_dim(
        jnp.zeros((3 * rank, width), F32), error_part, row_first, 1
    )
    pick = (
        lax.broadcasted_iota(jnp.int32, (width, rows), 0)
        == row_first + lax.broadcasted_iota(jnp.int32, (width, rows), 1)
    ).astype(BF)

    slots = ((0, 0), (0, 1), (3, 0), (1, 0))
    partial = ahead(slots, t_roll, c_roll, (low, high, left_low, right_low))
    partial = ahead(((3, 1), (1, 1)), t_roll, c_roll, (left_high, right_high), partial)
    wide = 3 * half
    block = pl.BlockSpec((tok, wide), lambda k: (k, 0))
    piece = pl.BlockSpec((2 * rows, wide), lambda k: (0, 0))
    across = pl.BlockSpec((1, 4, rows, tok), lambda k: (2, 0, 0, k))

    def slot(b):
        return pl.BlockSpec((4, 1, rows, tok), lambda k: (0, b, 0, k))

    def fixed(*shape):
        return pl.BlockSpec(shape, lambda k: (0,) * len(shape))

    line = fixed(4 * rows, wide)
    mine = (groups, 3 * rank // groups, width)
    grads, far_own, far_other, power = call(
        functools.partial(late_body, grad_scale, groups),
        (struct((2 * tok, wide)), struct((4 * rows, wide)), struct((4 * rows, wide)), struct(mine)),
        grid=(2,),
        ins=[block, across, across, piece, piece, fixed(3, rank, half), slot(2), slot(2)]
        + [fixed(tok, width)] * 4
        + [fixed(3 * rank, width)],
        outs=(block, line, line, fixed(*mine)),
        scratch=[pltpu.VMEM((3 * rank, width), F32)],
        flops=2 * 2 * tok * 8 * rows * wide,
        vmem=44,
    )(
        partial, t_roll, c_roll, over_low, over_high, q_rows.astype(BF), t_roll, c_roll,
        tokens, other_t, cotangent, other_c, placed,
    )

    one_own, one_other, three_own, three_other = call(
        near_body,
        (struct((4 * rows, wide)),) * 4,
        grid=(2,),
        ins=[slot(1), slot(1), slot(3), slot(3), block],
        outs=(line,) * 4,
        flops=2 * 2 * tok * 8 * rows * wide,
        vmem=32,
    )(t_roll, c_roll, t_roll, c_roll, grads)

    def relay(send, away_own, away_other, one_own, one_other, three_own, three_other):
        to_right, to_left = send(away_own, 1), send(away_other, -1)
        left_other, right_own = send(one_other, 1), send(three_own, -1)
        left_own = send((one_own.astype(F32) + to_right.astype(F32)).astype(BF), 1)
        right_other = send((three_other.astype(F32) + to_left.astype(F32)).astype(BF), -1)
        return right_own, right_other, left_own, left_other

    terms = relay(first, far_own, far_other, one_own, one_other, three_own, three_other)
    sums = call(
        home_body,
        (struct((rows, wide)),) * 8,
        grid=(2,),
        ins=[slot(0), slot(0), block] + [line] * 4,
        outs=(fixed(rows, wide),) * 8,
        flops=2 * 2 * tok * 4 * rows * wide,
        vmem=32,
    )(t_roll, c_roll, grads, *terms)
    own_sums, other_sums = sums[:4], sums[4:]
    right_own, right_other, left_own, left_other = relay(
        second, own_sums[2], other_sums[2], own_sums[1], other_sums[1], own_sums[3], other_sums[3]
    )

    def total(value, a, b):
        return (value.astype(F32) + a.astype(F32) + b.astype(F32)).astype(BF)

    kept = total(own_sums[0], right_own, left_own)
    sent = other_core(total(other_sums[0], right_other, left_other))

    power = spread(exchange(power, GRP), node_count)
    power = spread(exchange(power, NODE), groups)
    power = exchange(power, GRP)

    tiles = call(
        functools.partial(right_body, grad_scale, groups),
        struct((4, 3 * rank, half // 4)),
        flops=4 * 3 * rank * 2 * tok * width,
        vmem=20,
    )(power, tokens, other_t, cotangent, other_c, grads, error_sum.astype(BF), pick)
    tiles = spread(exchange(tiles, Z), node_count)
    tiles = spread(exchange(tiles, NODE), groups)
    tiles = exchange(tiles, (C, Z))
    inverse, hats = call(
        factor_body, (struct((3, rank, rank), F32), struct((3, rank, rows), F32)), flops=1 << 24, vmem=8
    )(power, pick)

    pieces = (low, high, right_low, right_high, over_low, over_high, left_low, left_high)
    token_own, token_other = call(
        token_body,
        (struct((node_count, rows, tok)),) * 2,
        ins=[SCALAR] + [WHOLE] * 9,
        flops=2 * 2 * tok * width * 2 * half,
        vmem=20,
    )(order, grads, *pieces)
    token_grad = call(turn_body, struct((tok, width)), vmem=16)(
        token_own.reshape(width, tok), other_core(token_other).reshape(width, tok)
    )

    new_error, q_new = call(
        functools.partial(final_body, grad_scale),
        (struct((1, rows, 3 * units)), struct((3, rank, units), F32)),
        ins=[SCALAR] + [WHOLE] * 6,
        vmem=16,
    )(core.reshape(1).astype(jnp.int32), tiles, inverse, hats, kept, sent, error)
    return (token_grad, new_error, jnp.swapaxes(hats, 1, 2), jnp.swapaxes(q_new, 1, 2))


def solution(mesh):
    finer = Mesh(mesh.devices.reshape(4, 4, 4, 2), NODE_GRP)
    placed = (
        P(NODE_GRP, None),
        P(NODE_GRP, None),
        P(NODE, None),
        P(NODE, None),
        P(NODE, None),
        P(GRP, NODE, None),
        P(),
    )
    return jax.shard_map(
        on_device,
        mesh=finer,
        in_specs=placed,
        out_specs=(P(NODE_GRP, None), P(GRP, NODE, None), P(None, NODE, None), P()),
        check_vma=False,
    )
```

```python
import functools
import math

import jax
import jax.numpy as jnp
from jax import lax
from jax.experimental import pallas as pl
from jax.experimental.pallas import tpu as pltpu
from jax.sharding import Mesh
from jax.sharding import PartitionSpec as P

Y, X, Z, C = "node_0", "node_1", "grp_0", "grp_1"
NODE = (Y, X)
GRP = (Z, C)
NODE_GRP = (Y, X, Z, C)
BF = jnp.bfloat16
F32 = jnp.float32
HIGH = lax.Precision.HIGHEST


def neighbour(value, stage, by):
    pairs = []
    for device in range(128):
        y, x, z, c = device // 32, device // 8 % 4, device // 2 % 4, device % 2
        if (c == 0) == (stage == 0):
            to = (y, (x + by) % 4, z, c)
        else:
            to = ((y + by) % 4, x, z, c)
        pairs.append((device, to[0] * 32 + to[1] * 8 + to[2] * 2 + to[3]))
    return lax.ppermute(value, NODE_GRP, pairs)


def other_core(value):
    return lax.ppermute(value, C, [(0, 1), (1, 0)])


def exchange(tiles, axis):
    return lax.all_to_all(tiles, axis, split_axis=0, concat_axis=0, tiled=True)


def dot(a, b, ca=1, cb=0, precision=None):
    return lax.dot_general(
        a, b, (((ca,), (cb,)), ((), ())), precision=precision, preferred_element_type=F32
    )


def call(body, out, grid=None, ins=None, outs=None, flops=0, scratch=(), vmem=24):
    params = {}
    if grid is not None:
        params.update(grid=grid, in_specs=ins, out_specs=outs)
    elif ins is not None:
        params.update(in_specs=ins)
    if flops:
        params["cost_estimate"] = pl.CostEstimate(
            flops=flops, bytes_accessed=1 << 20, transcendentals=0
        )
    return pl.pallas_call(
        body,
        out_shape=out,
        scratch_shapes=scratch,
        compiler_params=pltpu.CompilerParams(vmem_limit_bytes=(vmem + vmem // 2 + 6) << 20),
        **params,
    )


SCALAR = pl.BlockSpec(memory_space=pltpu.SMEM)
WHOLE = pl.BlockSpec(memory_space=pltpu.VMEM)


def struct(shape, kind=BF):
    return jax.ShapeDtypeStruct(shape, kind)


def near_struct(shape, kind=BF):
    return pltpu.VMEM(shape, kind)


def far_struct(shape, kind=BF):
    return pltpu.HBM(shape, kind)


def far(*values):
    return tuple(pltpu.with_memory_space_constraint(v, pltpu.HBM) for v in values)


def near(*values):
    return tuple(pltpu.with_memory_space_constraint(v, pltpu.VMEM) for v in values)


def gelu_parts(value):
    coeff = math.sqrt(2.0 / math.pi)
    inner = coeff * (value + 0.044715 * value * value * value)
    tanh_value = jnp.tanh(inner)
    activation = 0.5 * value * (1.0 + tanh_value)
    slope = 0.5 * (1.0 + tanh_value) + 0.5 * value * (1.0 - tanh_value * tanh_value) * coeff * (
        1.0 + 3.0 * 0.044715 * value * value
    )
    return (activation, slope)


def start_body(place_ref, gate_ref, up_ref, down_ref, own_ref):
    half = gate_ref.shape[1] // 2
    core = place_ref[16]
    for m, ref in enumerate((gate_ref, up_ref, down_ref)):
        own_ref[:, m * half : (m + 1) * half] = ref[:, pl.ds(pl.multiple_of(core * half, 128), half)]


def error_body(place_ref, e_ref, mine_ref, send_ref):
    half = mine_ref.shape[1] // 3
    units = 2 * half
    core = place_ref[16]
    for m in range(3):
        at = m * units + core * half
        mine_ref[:, m * half : (m + 1) * half] = e_ref[:, pl.ds(pl.multiple_of(at, 128), half)]
        at = m * units + (1 - core) * half
        send_ref[:, m * half : (m + 1) * half] = e_ref[:, pl.ds(pl.multiple_of(at, 128), half)]


def low_body(own_ref, left_ref, right_ref, low_ref, far_low_ref, far_high_ref):
    rows, at = own_ref.shape[0], far_low_ref.shape[0]
    low_ref[:rows] = own_ref[...]
    low_ref[rows:] = right_ref[...]
    far_low_ref[...] = left_ref[:at]
    far_high_ref[...] = right_ref[at:]


def high_body(far_low_ref, far_high_ref, left_ref, high_ref):
    at, rows = far_low_ref.shape[0], left_ref.shape[0]
    high_ref[:at] = far_low_ref[...]
    high_ref[at:rows] = far_high_ref[...]
    high_ref[rows:] = left_ref[...]


def picked(place_ref, width, rows):
    here = lax.broadcasted_iota(jnp.int32, (width, rows), 0) - place_ref[17]
    return jnp.where(here == lax.broadcasted_iota(jnp.int32, (width, rows), 1), 1.0, 0.0).astype(BF)


def roll_body(order_ref, own_ref, other_ref, out_ref, both_ref, scratch):
    tok, rows = own_ref.shape[0], out_ref.shape[1]
    both_ref[:tok] = own_ref[...]
    both_ref[tok:] = other_ref[...]
    scratch[:, :tok] = own_ref[...].T
    scratch[:, tok:] = other_ref[...].T
    for s in range(out_ref.shape[0]):
        out_ref[s] = scratch[pl.ds(pl.multiple_of(order_ref[s] * rows, 16), rows), :]


def rolled(order, own, other, rows):
    tok, width = own.shape
    roll, both = call(
        roll_body,
        (near_struct((width // rows, rows, 2 * tok)), near_struct((2 * tok, width))),
        ins=[SCALAR, WHOLE, WHOLE],
        scratch=[pltpu.VMEM((width, 2 * tok), BF)],
        vmem=5,
    )(order, own, other)
    return roll, both


def pair(ref, a, b, tok):
    at = pl.multiple_of(pl.program_id(0) * tok, 128)
    value = ref[4 * a + 2 * b : 4 * a + 2 * b + 2, :, pl.ds(at, tok)]
    return value.reshape(-1, tok)


def line(ref, b, tok):
    at = pl.multiple_of(pl.program_id(0) * tok, 128)
    return jnp.concatenate([ref[4 * a + b, :, pl.ds(at, tok)] for a in range(4)], axis=0)


def joined(ref):
    return ref[...].reshape(-1, ref.shape[-1])


def tokens_of(ref, tok):
    return ref.at[pl.ds(pl.multiple_of(pl.program_id(0) * tok, 128), tok), :]


def ahead_body(slots, t_ref, c_ref, *refs):
    tok = t_ref.shape[2] // 2
    out_ref = tokens_of(refs[-1], tok)
    units = out_ref.shape[-1] // 3
    gate_up, back = 0.0, 0.0
    if len(refs) > len(slots) + 1:
        part = tokens_of(refs[-2], tok)
        gate_up, back = part[:, : 2 * units], part[:, 2 * units :]
    for (a, b), piece in zip(slots, refs):
        gate_up = gate_up + dot(pair(t_ref, a, b, tok), piece[:, : 2 * units], 0, 0)
        back = back + dot(pair(c_ref, a, b, tok), piece[:, 2 * units :], 0, 0)
    out_ref[:, : 2 * units] = gate_up
    out_ref[:, 2 * units :] = back


def ahead(slots, t_roll, c_roll, pieces, partial=None):
    both, wide = t_roll.shape[2], pieces[0].shape[1]
    more = () if partial is None else near(partial)
    return call(
        functools.partial(ahead_body, slots),
        near_struct((both, wide), F32),
        grid=(2,),
        ins=[WHOLE] * (2 + len(pieces) + len(more)),
        outs=WHOLE,
        flops=2 * both * wide * pieces[0].shape[0] * len(pieces),
        vmem=5,
    )(*near(t_roll, c_roll), *pieces, *more)


def weight_part(t, c, grads):
    units = grads.shape[1] // 3
    return jnp.concatenate([dot(t, grads[:, : 2 * units]), dot(c, grads[:, 2 * units :])], axis=1)


def late_body(
    scale, groups, place_ref, part_all, t_ref, c_ref, low, high, q_ref, t_both, c_both,
    e_ref, e_other_ref, grads_ref, far_own, far_other, power_ref, total
):
    tok = t_ref.shape[2] // 2
    part_ref = tokens_of(part_all, tok)
    units = grads_ref.shape[-1] // 3
    gate_up, back = part_ref[:, : 2 * units], part_ref[:, 2 * units :]
    for b, piece in enumerate((low, high)):
        gate_up = gate_up + dot(pair(t_ref, 2, b, tok), piece[:, : 2 * units], 0, 0)
        back = back + dot(pair(c_ref, 2, b, tok), piece[:, 2 * units :], 0, 0)
    up_pre = gate_up[:, units:]
    activation, slope = gelu_parts(gate_up[:, :units])
    parts = (back * up_pre * slope, back * activation, activation * up_pre)
    parts = [part.astype(BF) for part in parts]
    for m, part in enumerate(parts):
        grads_ref[:, m * units : (m + 1) * units] = part
    far = weight_part(line(t_ref, 2, tok), line(c_ref, 2, tok), grads_ref).astype(BF)
    first = jnp.concatenate([dot(q_ref[m], parts[m], 1, 1) for m in range(2)], axis=0).astype(BF)
    second = dot(q_ref[2], parts[2], 1, 1).astype(BF)
    split = first.shape[0]
    top, bottom = dot(first, tokens_of(t_both, tok)[...]), dot(second, tokens_of(c_both, tok)[...])

    def start():
        far_own[...] = far
        total[:split], total[split:] = top, bottom

    def finish():
        far_other[...] = far
        value = jnp.concatenate([top + total[:split], bottom + total[split:]], axis=0)
        width, rows = value.shape[1], e_ref.shape[0]
        error = e_ref[...].astype(F32) + e_other_ref[...].astype(F32)
        error = jnp.concatenate(
            [dot(q_ref[m].astype(F32), error[:, m * units : (m + 1) * units], 1, 1) for m in range(3)],
            axis=0,
        )
        error_high = error.astype(BF)
        error_low = (error - error_high.astype(F32)).astype(BF)
        pick = picked(place_ref, width, rows)
        placed = dot(error_high, pick, 1, 1) + dot(error_low, pick, 1, 1)
        value = (value * scale + placed) * (1.0 / groups)
        step = value.shape[0] // groups
        for i in range(groups):
            power_ref[i] = value[i * step : (i + 1) * step].astype(BF)

    pl.when(pl.program_id(0) == 0)(start)
    pl.when(pl.program_id(0) == 1)(finish)


def near_body(t_one, c_one, t_three, c_three, grads_ref, *outs):
    one = weight_part(joined(t_one), joined(c_one), grads_ref).astype(BF)
    three = weight_part(joined(t_three), joined(c_three), grads_ref).astype(BF)
    for k in range(2):

        def put(k=k):
            outs[k][...] = one
            outs[2 + k][...] = three

        pl.when(pl.program_id(0) == k)(put)


def home_body(t_ref, c_ref, grads_ref, right_own, right_other, left_own, left_other, *outs):
    value = weight_part(joined(t_ref), joined(c_ref), grads_ref)
    rows = outs[0].shape[0]

    def put(k, a, b):
        total = (value + a[...].astype(F32) + b[...].astype(F32)).astype(BF)
        for i in range(4):
            outs[4 * k + i][...] = total[i * rows : (i + 1) * rows]

    pl.when(pl.program_id(0) == 0)(lambda: put(0, right_own, left_own))
    pl.when(pl.program_id(0) == 1)(lambda: put(1, right_other, left_other))


def spread_body(in_ref, out_ref):
    total = in_ref[0].astype(F32)
    for i in range(1, in_ref.shape[0]):
        total = total + in_ref[i].astype(F32)
    total = total.astype(BF)
    for i in range(out_ref.shape[0]):
        out_ref[i] = total


def spread(tiles, count):
    return call(spread_body, far_struct((count, *tiles.shape[1:])), vmem=4)(tiles)


def stacked(p_ref):
    return jnp.concatenate([p_ref[i].astype(F32) for i in range(p_ref.shape[0])], axis=0)


def right_body(
    scale, groups, place_ref, p_ref, t_ref, c_ref, y_ref, e_ref, e_other_ref, out_ref, total
):
    power = stacked(p_ref).astype(BF)
    rank = power.shape[0] // 3
    units = y_ref.shape[1] // 3
    seen = dot(power[: 2 * rank], t_ref[...], 1, 1).astype(BF)
    lhs = (seen[:rank], seen[rank:], dot(power[2 * rank :], c_ref[...], 1, 1).astype(BF))
    values = [dot(lhs[m], y_ref[:, m * units : (m + 1) * units]) for m in range(3)]

    def start():
        for m in range(3):
            total[m] = values[m]

    def finish():
        rows = dot(power, picked(place_ref, power.shape[1], e_ref.shape[0])).astype(BF)
        error = (e_ref[...].astype(F32) + e_other_ref[...].astype(F32)).astype(BF)
        for m in range(3):
            value = (values[m] + total[m]) * scale
            value = value + dot(
                rows[m * rank : (m + 1) * rank], error[:, m * units : (m + 1) * units]
            )
            value = (value * (1.0 / groups)).astype(BF)
            step = units // 4
            for i in range(4):
                out_ref[i, m * rank : (m + 1) * rank] = value[:, i * step : (i + 1) * step]

    pl.when(pl.program_id(0) == 0)(start)
    pl.when(pl.program_id(0) == 1)(finish)


def factor_body(place_ref, p_ref, inverse_ref, hats_ref):
    power = stacked(p_ref)
    r = power.shape[0] // 3
    low = power.astype(BF)
    gram = jnp.stack(
        [dot(low[m * r : (m + 1) * r], low[m * r : (m + 1) * r], 1, 1) for m in range(3)]
    )
    rows = lax.broadcasted_iota(jnp.int32, (3, r, 2 * r), 1)
    cols = lax.broadcasted_iota(jnp.int32, (3, r, 2 * r), 2)
    both = jnp.concatenate([gram, jnp.zeros((3, r, r), F32)], axis=2)
    both = both + jnp.where(cols == rows + r, 1.0, 0.0)
    for j in range(r):
        column = jnp.where(rows[:, :, :1] > j, both[:, :, j : j + 1], 0.0)
        row = both[:, j : j + 1, :] / both[:, j : j + 1, j : j + 1]
        both = both - column * row
    diagonal = jnp.sum(jnp.where(cols == rows, both, 0.0), axis=2, keepdims=True)
    inverse = both[:, :, r:] * (1.0 / jnp.sqrt(diagonal))
    inverse_ref[...] = inverse
    mine = dot(low, picked(place_ref, low.shape[1], hats_ref.shape[2]))
    for m in range(3):
        hats_ref[m] = dot(inverse[m], mine[m * r : (m + 1) * r], 1, 0, HIGH)


def final_body(scale, core_ref, b_ref, inverse_ref, hats_ref, kept_ref, sent_ref, e_ref, err_ref, q_ref):
    r = inverse_ref.shape[1]
    units = q_ref.shape[2]
    half = units // 2
    core = core_ref[16]
    for m in range(3):
        right = jnp.concatenate(
            [b_ref[i, m * r : (m + 1) * r].astype(F32) for i in range(b_ref.shape[0])], axis=1
        )
        q_t = dot(inverse_ref[m], right, 1, 0, HIGH)
        q_ref[m] = q_t
        rebuilt = dot(hats_ref[m].astype(BF), q_t.astype(BF), 0, 0)
        kept = kept_ref[:, m * half : (m + 1) * half].astype(F32)
        sent = sent_ref[:, m * half : (m + 1) * half].astype(F32)
        for side in range(2):
            at = slice(m * units + side * half, m * units + (side + 1) * half)
            grad = jnp.where(core == side, kept, sent)
            value = grad * scale + e_ref[:, at].astype(F32)
            err_ref[0, :, at] = (value - rebuilt[:, side * half : (side + 1) * half]).astype(BF)


def token_body(order_ref, y_ref, *refs):
    own_ref, other_ref = refs[-2:]
    rows, tok = own_ref.shape[1:]
    wide = y_ref.shape[1] // 3 * 2
    for s in range(0, own_ref.shape[0], 2):
        value = dot(refs[s // 2][:, :wide], y_ref[:, :wide], 1, 1).astype(BF)
        for i in range(2):
            at = order_ref[s + i]
            own_ref[at] = value[i * rows : (i + 1) * rows, :tok]
            other_ref[at] = value[i * rows : (i + 1) * rows, tok:]


def turn_body(a_ref, b_ref, out_ref):
    value = a_ref[...].astype(F32) + b_ref[...].astype(F32)
    out_ref[...] = value.T.astype(BF)


def on_device(tokens, cotangent, gate_weight, up_weight, down_weight_t, error_memory, q_init):
    yi, xi, core = lax.axis_index(Y), lax.axis_index(X), lax.axis_index(C)
    rows, units = gate_weight.shape
    node_count, groups = lax.axis_size(NODE), lax.axis_size(GRP)
    half, rank = units // 2, q_init.shape[-1]
    tok, width = tokens.shape
    grad_scale = 1.0 / math.sqrt(tok * node_count)

    def first(value, by):
        return neighbour(value, 0, by)

    def second(value, by):
        return neighbour(value, 1, by)

    over, along = jnp.arange(4)[:, None], jnp.arange(4)[None, :]
    ys = jnp.where(core == 0, yi + over, yi + along) % 4
    xs = jnp.where(core == 0, xi + along, xi + over) % 4
    place = jnp.concatenate(
        [(ys * 4 + xs).reshape(-1), core.reshape(1), ((yi * 4 + xi) * rows).reshape(1)]
    ).astype(jnp.int32)

    wide = 3 * half
    error = error_memory[0]
    weights = [
        pltpu.with_memory_space_constraint(w, pltpu.HBM)
        for w in (gate_weight, up_weight, down_weight_t)
    ]
    own = call(start_body, struct((rows, wide)), ins=[SCALAR] + [WHOLE] * 3, vmem=3)(place, *weights)
    from_left, from_right = first(own, 1), first(own, -1)
    other_t, other_c = other_core(tokens), other_core(cotangent)
    e_mine, e_send = call(
        error_body, (struct((rows, wide)),) * 2, ins=[SCALAR, WHOLE], vmem=3
    )(place, error)
    e_other = other_core(e_send)
    t_roll, t_both = rolled(place, tokens, other_t, rows)
    from_left, from_right, t_roll = lax.optimization_barrier((from_left, from_right, t_roll))
    at = rows // 32 * 16
    low, far_low, far_high = call(
        low_body,
        (struct((2 * rows, wide)), struct((at, wide)), struct((rows - at, wide))),
        vmem=2,
    )(own, from_left, from_right)
    far_low, far_high = first(far_low, 1), first(far_high, -1)
    left_low, right_low = second(low, 1), second(low, -1)
    c_roll, c_both = rolled(place, cotangent, other_c, rows)
    high = call(high_body, struct((2 * rows, wide)), vmem=2)(far_low, far_high, from_left)
    left_high = second(high, 1)
    right_high = second(high, -1)
    over_low, over_high = second(left_low, 1), second(right_high, -1)
    q_rows = lax.dynamic_slice_in_dim(jnp.swapaxes(q_init, 1, 2), core * half, half, 2).astype(BF)

    partial = ahead(((0, 0), (0, 1)), t_roll, c_roll, (low, high))
    slots = ((3, 0), (1, 0), (3, 1), (1, 1))
    partial = ahead(slots, t_roll, c_roll, (left_low, right_low, left_high, right_high), partial)
    long, mine = (4 * rows, wide), (groups, 3 * rank // groups, width)
    block = pl.BlockSpec((tok, wide), lambda k: (k, 0))

    def slot(b):
        return pl.BlockSpec((4, 1, rows, tok), lambda k: (0, b, 0, k))

    def fixed(*shape):
        return pl.BlockSpec(shape, lambda k: (0,) * len(shape))

    grads, far_own, far_other, power = call(
        functools.partial(late_body, grad_scale, groups),
        (far_struct((2 * tok, wide)), far_struct(long), far_struct(long), far_struct(mine)),
        grid=(2,),
        ins=[SCALAR] + [WHOLE] * 10,
        outs=(block, fixed(*long), fixed(*long), fixed(*mine)),
        scratch=[pltpu.VMEM((3 * rank, width), F32)],
        flops=2 * 2 * tok * 8 * rows * wide,
        vmem=16,
    )(
        place, *near(partial, t_roll, c_roll), over_low, over_high, q_rows, *near(t_both, c_both),
        e_mine, e_other,
    )

    four = (4, 4, rows, 2 * tok)
    rolls = far(t_roll.reshape(four), c_roll.reshape(four))
    one_own, one_other, three_own, three_other = call(
        near_body,
        (far_struct(long),) * 4,
        grid=(2,),
        ins=[slot(1), slot(1), slot(3), slot(3), block],
        outs=(fixed(*long),) * 4,
        flops=2 * 2 * tok * 8 * rows * wide,
        vmem=16,
    )(*rolls, *rolls, *far(grads))

    power = spread(exchange(power, GRP), node_count)
    power, one_other, three_own = lax.optimization_barrier((power, one_other, three_own))
    power = spread(exchange(power, NODE), groups)
    power = exchange(power, GRP)

    def relay(send, away_own, away_other, one_own, one_other, three_own, three_other):
        to_right, to_left = send(away_own, 1), send(away_other, -1)
        left_other, right_own = send(one_other, 1), send(three_own, -1)
        left_own = send((one_own.astype(F32) + to_right.astype(F32)).astype(BF), 1)
        right_other = send((three_other.astype(F32) + to_left.astype(F32)).astype(BF), -1)
        return right_own, right_other, left_own, left_other

    terms = relay(first, far_own, far_other, one_own, one_other, three_own, three_other)
    sums = call(
        home_body,
        (far_struct((rows, wide)),) * 8,
        grid=(2,),
        ins=[slot(0), slot(0), block] + [fixed(*long)] * 4,
        outs=(fixed(rows, wide),) * 8,
        flops=2 * 2 * tok * 4 * rows * wide,
        vmem=16,
    )(*rolls, *far(grads), *far(*terms))
    own_sums, other_sums = sums[:4], sums[4:]
    right_own, right_other, left_own, left_other = relay(
        second, own_sums[2], other_sums[2], own_sums[1], other_sums[1], own_sums[3], other_sums[3]
    )

    def total(value, a, b):
        return (value.astype(F32) + a.astype(F32) + b.astype(F32)).astype(BF)

    kept = total(own_sums[0], right_own, left_own)
    sent = other_core(total(other_sums[0], right_other, left_other))

    tiles = call(
        functools.partial(right_body, grad_scale, groups),
        struct((4, 3 * rank, half // 4)),
        grid=(2,),
        ins=[SCALAR, WHOLE] + [pl.BlockSpec((tok, width), lambda k: (k, 0))] * 2 + [block, WHOLE, WHOLE],
        outs=fixed(4, 3 * rank, half // 4),
        scratch=[pltpu.VMEM((3, rank, half), F32)],
        flops=4 * 3 * rank * 2 * tok * width,
        vmem=12,
    )(place, power, *far(t_both, c_both, grads), e_mine, e_other)
    tiles = spread(exchange(tiles, Z), node_count)
    tiles = spread(exchange(tiles, NODE), groups)
    tiles = exchange(tiles, (C, Z))
    inverse, hats = call(
        factor_body,
        (struct((3, rank, rank), F32), struct((3, rank, rows), F32)),
        ins=[SCALAR, WHOLE],
        flops=1 << 24,
        vmem=2,
    )(place, power)

    pieces = (low, high, right_low, right_high, over_low, over_high, left_low, left_high)
    token_own, token_other = call(
        token_body,
        (struct((node_count, rows, tok)),) * 2,
        ins=[SCALAR] + [WHOLE] * 9,
        flops=2 * 2 * tok * width * 2 * half,
        vmem=12,
    )(place, *far(grads, *pieces))
    token_grad = call(turn_body, struct((tok, width)), vmem=4)(
        token_own.reshape(width, tok), other_core(token_other).reshape(width, tok)
    )

    new_error, q_new = call(
        functools.partial(final_body, grad_scale),
        (struct((1, rows, 3 * units)), struct((3, rank, units), F32)),
        ins=[SCALAR] + [WHOLE] * 6,
        vmem=3,
    )(place, tiles, inverse, hats, kept, sent, error)
    return (token_grad, new_error, jnp.swapaxes(hats, 1, 2), jnp.swapaxes(q_new, 1, 2))


def solution(mesh):
    finer = Mesh(mesh.devices.reshape(4, 4, 4, 2), NODE_GRP)
    placed = (
        P(NODE_GRP, None),
        P(NODE_GRP, None),
        P(NODE, None),
        P(NODE, None),
        P(NODE, None),
        P(GRP, NODE, None),
        P(),
    )

    return jax.shard_map(
        on_device,
        mesh=finer,
        in_specs=placed,
        out_specs=(P(NODE_GRP, None), P(GRP, NODE, None), P(None, NODE, None), P()),
        check_vma=False,
    )
```

```python
import functools
import math

import jax
import jax.numpy as jnp
from jax import lax
from jax.experimental import pallas as pl
from jax.experimental.pallas import tpu as pltpu
from jax.sharding import Mesh
from jax.sharding import PartitionSpec as P

Y, X, Z, C = "node_0", "node_1", "grp_0", "grp_1"
NODE = (Y, X)
GRP = (Z, C)
NODE_GRP = (Y, X, Z, C)
BF = jnp.bfloat16
F32 = jnp.float32
HIGH = lax.Precision.HIGHEST


def neighbour(value, stage, by):
    pairs = []
    for device in range(128):
        y, x, z, c = device // 32, device // 8 % 4, device // 2 % 4, device % 2
        if (c == 0) == (stage == 0):
            to = (y, (x + by) % 4, z, c)
        else:
            to = ((y + by) % 4, x, z, c)
        pairs.append((device, to[0] * 32 + to[1] * 8 + to[2] * 2 + to[3]))
    return lax.ppermute(value, NODE_GRP, pairs)


def other_core(value):
    return lax.ppermute(value, C, [(0, 1), (1, 0)])


def exchange(tiles, axis):
    return lax.all_to_all(tiles, axis, split_axis=0, concat_axis=0, tiled=True)


def dot(a, b, ca=1, cb=0, precision=None):
    return lax.dot_general(
        a, b, (((ca,), (cb,)), ((), ())), precision=precision, preferred_element_type=F32
    )


def call(body, out, grid=None, ins=None, outs=None, flops=0, scratch=(), vmem=24):
    params = {}
    if grid is not None:
        params.update(grid=grid, in_specs=ins, out_specs=outs)
    elif ins is not None:
        params.update(in_specs=ins)
    if flops:
        params["cost_estimate"] = pl.CostEstimate(
            flops=flops, bytes_accessed=1 << 20, transcendentals=0
        )
    return pl.pallas_call(
        body,
        out_shape=out,
        scratch_shapes=scratch,
        compiler_params=pltpu.CompilerParams(vmem_limit_bytes=(vmem + vmem // 2 + 6) << 20),
        **params,
    )


SCALAR = pl.BlockSpec(memory_space=pltpu.SMEM)
WHOLE = pl.BlockSpec(memory_space=pltpu.VMEM)


def struct(shape, kind=BF):
    return jax.ShapeDtypeStruct(shape, kind)


def near_struct(shape, kind=BF):
    return pltpu.VMEM(shape, kind)


def far_struct(shape, kind=BF):
    return pltpu.HBM(shape, kind)


def far(*values):
    return tuple(pltpu.with_memory_space_constraint(v, pltpu.HBM) for v in values)


def near(*values):
    return tuple(pltpu.with_memory_space_constraint(v, pltpu.VMEM) for v in values)


def gelu_parts(value):
    coeff = math.sqrt(2.0 / math.pi)
    inner = coeff * (value + 0.044715 * value * value * value)
    tanh_value = jnp.tanh(inner)
    activation = 0.5 * value * (1.0 + tanh_value)
    slope = 0.5 * (1.0 + tanh_value) + 0.5 * value * (1.0 - tanh_value * tanh_value) * coeff * (
        1.0 + 3.0 * 0.044715 * value * value
    )
    return (activation, slope)


def start_body(place_ref, gate_ref, up_ref, down_ref, own_ref):
    half = gate_ref.shape[1] // 2
    core = place_ref[16]
    for m, ref in enumerate((gate_ref, up_ref, down_ref)):
        own_ref[:, m * half : (m + 1) * half] = ref[:, pl.ds(pl.multiple_of(core * half, 128), half)]


def error_body(place_ref, e_ref, mine_ref, send_ref):
    half = mine_ref.shape[1] // 3
    units = 2 * half
    core = place_ref[16]
    for m in range(3):
        at = m * units + core * half
        mine_ref[:, m * half : (m + 1) * half] = e_ref[:, pl.ds(pl.multiple_of(at, 128), half)]
        at = m * units + (1 - core) * half
        send_ref[:, m * half : (m + 1) * half] = e_ref[:, pl.ds(pl.multiple_of(at, 128), half)]


def low_body(own_ref, left_ref, right_ref, low_ref, far_low_ref, far_high_ref):
    rows, at = own_ref.shape[0], far_low_ref.shape[0]
    low_ref[:rows] = own_ref[...]
    low_ref[rows:] = right_ref[...]
    far_low_ref[...] = left_ref[:at]
    far_high_ref[...] = right_ref[at:]


def high_body(far_low_ref, far_high_ref, left_ref, high_ref):
    at, rows = far_low_ref.shape[0], left_ref.shape[0]
    high_ref[:at] = far_low_ref[...]
    high_ref[at:rows] = far_high_ref[...]
    high_ref[rows:] = left_ref[...]


def picked(place_ref, width, rows):
    here = lax.broadcasted_iota(jnp.int32, (width, rows), 0) - place_ref[17]
    return jnp.where(here == lax.broadcasted_iota(jnp.int32, (width, rows), 1), 1.0, 0.0).astype(BF)


def roll_body(order_ref, own_ref, other_ref, out_ref, both_ref, scratch):
    tok, rows = own_ref.shape[0], out_ref.shape[1]
    both_ref[:tok] = own_ref[...]
    both_ref[tok:] = other_ref[...]
    scratch[:, :tok] = own_ref[...].T
    scratch[:, tok:] = other_ref[...].T
    for s in range(out_ref.shape[0]):
        out_ref[s] = scratch[pl.ds(pl.multiple_of(order_ref[s] * rows, 16), rows), :]


def rolled(order, own, other, rows):
    tok, width = own.shape
    roll, both = call(
        roll_body,
        (near_struct((width // rows, rows, 2 * tok)), near_struct((2 * tok, width))),
        ins=[SCALAR, WHOLE, WHOLE],
        scratch=[pltpu.VMEM((width, 2 * tok), BF)],
        vmem=5,
    )(order, own, other)
    return roll, both


def pair(ref, a, b, tok):
    at = pl.multiple_of(pl.program_id(0) * tok, 128)
    value = ref[4 * a + 2 * b : 4 * a + 2 * b + 2, :, pl.ds(at, tok)]
    return value.reshape(-1, tok)


def line(ref, b, tok):
    at = pl.multiple_of(pl.program_id(0) * tok, 128)
    return jnp.concatenate([ref[4 * a + b, :, pl.ds(at, tok)] for a in range(4)], axis=0)


def joined(ref):
    return ref[...].reshape(-1, ref.shape[-1])


def tokens_of(ref, tok):
    return ref.at[pl.ds(pl.multiple_of(pl.program_id(0) * tok, 128), tok), :]


def ahead_body(slots, t_ref, c_ref, *refs):
    tok = t_ref.shape[2] // 2
    out_ref = tokens_of(refs[-1], tok)
    units = out_ref.shape[-1] // 3
    gate_up, back = 0.0, 0.0
    if len(refs) > len(slots) + 1:
        part = tokens_of(refs[-2], tok)
        gate_up, back = part[:, : 2 * units], part[:, 2 * units :]
    for (a, b), piece in zip(slots, refs):
        gate_up = gate_up + dot(pair(t_ref, a, b, tok), piece[:, : 2 * units], 0, 0)
        back = back + dot(pair(c_ref, a, b, tok), piece[:, 2 * units :], 0, 0)
    out_ref[:, : 2 * units] = gate_up
    out_ref[:, 2 * units :] = back


def ahead(slots, t_roll, c_roll, pieces, partial=None):
    both, wide = t_roll.shape[2], pieces[0].shape[1]
    more = () if partial is None else near(partial)
    return call(
        functools.partial(ahead_body, slots),
        near_struct((both, wide), F32),
        grid=(2,),
        ins=[WHOLE] * (2 + len(pieces) + len(more)),
        outs=WHOLE,
        flops=2 * both * wide * pieces[0].shape[0] * len(pieces),
        vmem=5,
    )(*near(t_roll, c_roll), *pieces, *more)


def weight_part(t, c, grads):
    units = grads.shape[1] // 3
    return jnp.concatenate([dot(t, grads[:, : 2 * units]), dot(c, grads[:, 2 * units :])], axis=1)


def late_body(
    scale, groups, place_ref, part_all, t_ref, c_ref, low, high, q_ref, t_both, c_both,
    e_ref, e_other_ref, grads_ref, far_own, far_other, power_ref, total
):
    tok = t_ref.shape[2] // 2
    part_ref = tokens_of(part_all, tok)
    units = grads_ref.shape[-1] // 3
    gate_up, back = part_ref[:, : 2 * units], part_ref[:, 2 * units :]
    for b, piece in enumerate((low, high)):
        gate_up = gate_up + dot(pair(t_ref, 2, b, tok), piece[:, : 2 * units], 0, 0)
        back = back + dot(pair(c_ref, 2, b, tok), piece[:, 2 * units :], 0, 0)
    up_pre = gate_up[:, units:]
    activation, slope = gelu_parts(gate_up[:, :units])
    parts = (back * up_pre * slope, back * activation, activation * up_pre)
    parts = [part.astype(BF) for part in parts]
    for m, part in enumerate(parts):
        grads_ref[:, m * units : (m + 1) * units] = part
    far = weight_part(line(t_ref, 2, tok), line(c_ref, 2, tok), grads_ref).astype(BF)
    first = jnp.concatenate([dot(q_ref[m], parts[m], 1, 1) for m in range(2)], axis=0).astype(BF)
    second = dot(q_ref[2], parts[2], 1, 1).astype(BF)
    split = first.shape[0]
    top, bottom = dot(first, tokens_of(t_both, tok)[...]), dot(second, tokens_of(c_both, tok)[...])

    def start():
        far_own[...] = far
        total[:split], total[split:] = top, bottom

    def finish():
        far_other[...] = far
        value = jnp.concatenate([top + total[:split], bottom + total[split:]], axis=0)
        width, rows = value.shape[1], e_ref.shape[0]
        error = e_ref[...].astype(F32) + e_other_ref[...].astype(F32)
        error = jnp.concatenate(
            [dot(q_ref[m].astype(F32), error[:, m * units : (m + 1) * units], 1, 1) for m in range(3)],
            axis=0,
        )
        error_high = error.astype(BF)
        error_low = (error - error_high.astype(F32)).astype(BF)
        pick = picked(place_ref, width, rows)
        placed = dot(error_high, pick, 1, 1) + dot(error_low, pick, 1, 1)
        value = (value * scale + placed) * (1.0 / groups)
        step = width // groups
        for i in range(groups):
            power_ref[i] = value[:, i * step : (i + 1) * step].astype(BF)

    pl.when(pl.program_id(0) == 0)(start)
    pl.when(pl.program_id(0) == 1)(finish)


def near_body(t_one, c_one, t_three, c_three, grads_ref, *outs):
    one = weight_part(joined(t_one), joined(c_one), grads_ref).astype(BF)
    three = weight_part(joined(t_three), joined(c_three), grads_ref).astype(BF)
    for k in range(2):

        def put(k=k):
            outs[k][...] = one
            outs[2 + k][...] = three

        pl.when(pl.program_id(0) == k)(put)


def home_body(t_ref, c_ref, grads_ref, right_own, right_other, left_own, left_other, *outs):
    value = weight_part(joined(t_ref), joined(c_ref), grads_ref)
    rows = outs[0].shape[0]

    def put(k, a, b):
        total = (value + a[...].astype(F32) + b[...].astype(F32)).astype(BF)
        for i in range(4):
            outs[4 * k + i][...] = total[i * rows : (i + 1) * rows]

    pl.when(pl.program_id(0) == 0)(lambda: put(0, right_own, left_own))
    pl.when(pl.program_id(0) == 1)(lambda: put(1, right_other, left_other))


def spread_body(in_ref, out_ref):
    total = in_ref[0].astype(F32)
    for i in range(1, in_ref.shape[0]):
        total = total + in_ref[i].astype(F32)
    total = total.astype(BF)
    for i in range(out_ref.shape[0]):
        out_ref[i] = total


def spread(tiles, count):
    return call(spread_body, far_struct((count, *tiles.shape[1:])), vmem=4)(tiles)


def joined_lanes(p_ref):
    return jnp.concatenate([p_ref[i].astype(F32) for i in range(p_ref.shape[0])], axis=1).astype(BF)


def right_body(
    scale, groups, place_ref, p_ref, t_ref, c_ref, y_ref, e_ref, e_other_ref, out_ref, total
):
    power = joined_lanes(p_ref)
    rank = power.shape[0] // 3
    units = y_ref.shape[1] // 3
    seen = dot(power[: 2 * rank], t_ref[...], 1, 1).astype(BF)
    lhs = (seen[:rank], seen[rank:], dot(power[2 * rank :], c_ref[...], 1, 1).astype(BF))
    values = [dot(lhs[m], y_ref[:, m * units : (m + 1) * units]) for m in range(3)]

    def start():
        for m in range(3):
            total[m] = values[m]

    def finish():
        rows = dot(power, picked(place_ref, power.shape[1], e_ref.shape[0])).astype(BF)
        error = (e_ref[...].astype(F32) + e_other_ref[...].astype(F32)).astype(BF)
        for m in range(3):
            value = (values[m] + total[m]) * scale
            value = value + dot(
                rows[m * rank : (m + 1) * rank], error[:, m * units : (m + 1) * units]
            )
            value = (value * (1.0 / groups)).astype(BF)
            step = units // 4
            for i in range(4):
                out_ref[i, m * rank : (m + 1) * rank] = value[:, i * step : (i + 1) * step]

    pl.when(pl.program_id(0) == 0)(start)
    pl.when(pl.program_id(0) == 1)(finish)


def factor_body(place_ref, p_ref, inverse_ref, hats_ref):
    low = joined_lanes(p_ref)
    r = low.shape[0] // 3
    gram = jnp.stack(
        [dot(low[m * r : (m + 1) * r], low[m * r : (m + 1) * r], 1, 1) for m in range(3)]
    )
    rows = lax.broadcasted_iota(jnp.int32, (3, r, 2 * r), 1)
    cols = lax.broadcasted_iota(jnp.int32, (3, r, 2 * r), 2)
    both = jnp.concatenate([gram, jnp.zeros((3, r, r), F32)], axis=2)
    both = both + jnp.where(cols == rows + r, 1.0, 0.0)
    for j in range(r):
        column = jnp.where(rows[:, :, :1] > j, both[:, :, j : j + 1], 0.0)
        row = both[:, j : j + 1, :] / both[:, j : j + 1, j : j + 1]
        both = both - column * row
    diagonal = jnp.sum(jnp.where(cols == rows, both, 0.0), axis=2, keepdims=True)
    inverse = both[:, :, r:] * (1.0 / jnp.sqrt(diagonal))
    inverse_ref[...] = inverse
    mine = dot(low, picked(place_ref, low.shape[1], hats_ref.shape[2]))
    for m in range(3):
        hats_ref[m] = dot(inverse[m], mine[m * r : (m + 1) * r], 1, 0, HIGH)


def final_body(scale, core_ref, b_ref, inverse_ref, hats_ref, kept_ref, sent_ref, e_ref, err_ref, q_ref):
    r = inverse_ref.shape[1]
    units = q_ref.shape[2]
    half = units // 2
    core = core_ref[16]
    for m in range(3):
        right = jnp.concatenate(
            [b_ref[i, m * r : (m + 1) * r].astype(F32) for i in range(b_ref.shape[0])], axis=1
        )
        q_t = dot(inverse_ref[m], right, 1, 0, HIGH)
        q_ref[m] = q_t
        rebuilt = dot(hats_ref[m].astype(BF), q_t.astype(BF), 0, 0)
        kept = kept_ref[:, m * half : (m + 1) * half].astype(F32)
        sent = sent_ref[:, m * half : (m + 1) * half].astype(F32)
        for side in range(2):
            at = slice(m * units + side * half, m * units + (side + 1) * half)
            grad = jnp.where(core == side, kept, sent)
            value = grad * scale + e_ref[:, at].astype(F32)
            err_ref[0, :, at] = (value - rebuilt[:, side * half : (side + 1) * half]).astype(BF)


def token_body(order_ref, y_ref, *refs):
    own_ref, other_ref = refs[-2:]
    rows, tok = own_ref.shape[1:]
    wide = y_ref.shape[1] // 3 * 2
    for s in range(0, own_ref.shape[0], 2):
        value = dot(refs[s // 2][:, :wide], y_ref[:, :wide], 1, 1).astype(BF)
        for i in range(2):
            at = order_ref[s + i]
            own_ref[at] = value[i * rows : (i + 1) * rows, :tok]
            other_ref[at] = value[i * rows : (i + 1) * rows, tok:]


def turn_body(a_ref, b_ref, out_ref):
    value = a_ref[...].astype(F32) + b_ref[...].astype(F32)
    out_ref[...] = value.T.astype(BF)


def on_device(tokens, cotangent, gate_weight, up_weight, down_weight_t, error_memory, q_init):
    yi, xi, core = lax.axis_index(Y), lax.axis_index(X), lax.axis_index(C)
    rows, units = gate_weight.shape
    node_count, groups = lax.axis_size(NODE), lax.axis_size(GRP)
    half, rank = units // 2, q_init.shape[-1]
    tok, width = tokens.shape
    grad_scale = 1.0 / math.sqrt(tok * node_count)

    def first(value, by):
        return neighbour(value, 0, by)

    def second(value, by):
        return neighbour(value, 1, by)

    over, along = jnp.arange(4)[:, None], jnp.arange(4)[None, :]
    ys = jnp.where(core == 0, yi + over, yi + along) % 4
    xs = jnp.where(core == 0, xi + along, xi + over) % 4
    place = jnp.concatenate(
        [(ys * 4 + xs).reshape(-1), core.reshape(1), ((yi * 4 + xi) * rows).reshape(1)]
    ).astype(jnp.int32)

    wide = 3 * half
    error = error_memory[0]
    weights = [
        pltpu.with_memory_space_constraint(w, pltpu.HBM)
        for w in (gate_weight, up_weight, down_weight_t)
    ]
    own = call(start_body, struct((rows, wide)), ins=[SCALAR] + [WHOLE] * 3, vmem=3)(place, *weights)
    from_left, from_right = first(own, 1), first(own, -1)
    other_t, other_c = other_core(tokens), other_core(cotangent)
    e_mine, e_send = call(
        error_body, (struct((rows, wide)),) * 2, ins=[SCALAR, WHOLE], vmem=3
    )(place, error)
    e_other = other_core(e_send)
    t_roll, t_both = rolled(place, tokens, other_t, rows)
    from_left, from_right, t_roll = lax.optimization_barrier((from_left, from_right, t_roll))
    at = rows // 32 * 16
    low, far_low, far_high = call(
        low_body,
        (struct((2 * rows, wide)), struct((at, wide)), struct((rows - at, wide))),
        vmem=2,
    )(own, from_left, from_right)
    far_low = first(far_low, 1)
    far_high = first(far_high, -1)
    left_low = second(low, 1)
    right_low = second(low, -1)
    c_roll, c_both = rolled(place, cotangent, other_c, rows)
    high = call(high_body, struct((2 * rows, wide)), vmem=2)(far_low, far_high, from_left)
    left_high = second(high, 1)
    right_high = second(high, -1)
    over_low, over_high = second(left_low, 1), second(right_high, -1)
    q_rows = lax.dynamic_slice_in_dim(jnp.swapaxes(q_init, 1, 2), core * half, half, 2).astype(BF)

    slots = ((0, 0), (0, 1), (3, 0), (1, 0))
    partial = ahead(slots, t_roll, c_roll, (low, high, left_low, right_low))
    partial = ahead(((3, 1), (1, 1)), t_roll, c_roll, (left_high, right_high), partial)
    long, mine = (4 * rows, wide), (groups, 3 * rank, width // groups)
    block = pl.BlockSpec((tok, wide), lambda k: (k, 0))

    def slot(b):
        return pl.BlockSpec((4, 1, rows, tok), lambda k: (0, b, 0, k))

    def fixed(*shape):
        return pl.BlockSpec(shape, lambda k: (0,) * len(shape))

    grads, far_own, far_other, power = call(
        functools.partial(late_body, grad_scale, groups),
        (far_struct((2 * tok, wide)), far_struct(long), far_struct(long), far_struct(mine)),
        grid=(2,),
        ins=[SCALAR] + [WHOLE] * 10,
        outs=(block, fixed(*long), fixed(*long), fixed(*mine)),
        scratch=[pltpu.VMEM((3 * rank, width), F32)],
        flops=2 * 2 * tok * 8 * rows * wide,
        vmem=16,
    )(
        place, *near(partial, t_roll, c_roll), over_low, over_high, q_rows, *near(t_both, c_both),
        e_mine, e_other,
    )

    four = (4, 4, rows, 2 * tok)
    rolls = far(t_roll.reshape(four), c_roll.reshape(four))
    one_own, one_other, three_own, three_other = call(
        near_body,
        (far_struct(long),) * 4,
        grid=(2,),
        ins=[slot(1), slot(1), slot(3), slot(3), block],
        outs=(fixed(*long),) * 4,
        flops=2 * 2 * tok * 8 * rows * wide,
        vmem=16,
    )(*rolls, *rolls, *far(grads))

    power = spread(exchange(power, GRP), node_count)
    power, one_other, three_own = lax.optimization_barrier((power, one_other, three_own))
    power = spread(exchange(power, NODE), groups)
    power = exchange(power, GRP)

    def relay(send, away_own, away_other, one_own, one_other, three_own, three_other):
        to_right, to_left = send(away_own, 1), send(away_other, -1)
        left_other, right_own = send(one_other, 1), send(three_own, -1)
        left_own = send((one_own.astype(F32) + to_right.astype(F32)).astype(BF), 1)
        right_other = send((three_other.astype(F32) + to_left.astype(F32)).astype(BF), -1)
        return right_own, right_other, left_own, left_other

    terms = relay(first, far_own, far_other, one_own, one_other, three_own, three_other)
    sums = call(
        home_body,
        (far_struct((rows, wide)),) * 8,
        grid=(2,),
        ins=[slot(0), slot(0), block] + [fixed(*long)] * 4,
        outs=(fixed(rows, wide),) * 8,
        flops=2 * 2 * tok * 4 * rows * wide,
        vmem=16,
    )(*rolls, *far(grads), *far(*terms))
    own_sums, other_sums = sums[:4], sums[4:]
    right_own, right_other, left_own, left_other = relay(
        second, own_sums[2], other_sums[2], own_sums[1], other_sums[1], own_sums[3], other_sums[3]
    )

    def total(value, a, b):
        return (value.astype(F32) + a.astype(F32) + b.astype(F32)).astype(BF)

    kept = total(own_sums[0], right_own, left_own)
    sent = other_core(total(other_sums[0], right_other, left_other))

    tiles = call(
        functools.partial(right_body, grad_scale, groups),
        far_struct((4, 3 * rank, half // 4)),
        grid=(2,),
        ins=[SCALAR, WHOLE] + [pl.BlockSpec((tok, width), lambda k: (k, 0))] * 2 + [block] + [fixed(rows, wide)] * 2,
        outs=fixed(4, 3 * rank, half // 4),
        scratch=[pltpu.VMEM((3, rank, half), F32)],
        flops=4 * 3 * rank * 2 * tok * width,
        vmem=12,
    )(place, power, *far(t_both, c_both, grads, e_mine, e_other))
    tiles = spread(exchange(tiles, Z), node_count)
    tiles = spread(exchange(tiles, NODE), groups)
    tiles = exchange(tiles, (C, Z))
    inverse, hats = call(
        factor_body,
        (struct((3, rank, rank), F32), struct((3, rank, rows), F32)),
        ins=[SCALAR, WHOLE],
        flops=1 << 24,
        vmem=2,
    )(place, power)

    pieces = (low, high, right_low, right_high, over_low, over_high, left_low, left_high)
    token_own, token_other = call(
        token_body,
        (struct((node_count, rows, tok)),) * 2,
        ins=[SCALAR] + [WHOLE] * 9,
        flops=2 * 2 * tok * width * 2 * half,
        vmem=12,
    )(place, *far(grads, *pieces))
    token_grad = call(turn_body, struct((tok, width)), vmem=4)(
        token_own.reshape(width, tok), other_core(token_other).reshape(width, tok)
    )

    new_error, q_new = call(
        functools.partial(final_body, grad_scale),
        (struct((1, rows, 3 * units)), struct((3, rank, units), F32)),
        ins=[SCALAR] + [WHOLE] * 6,
        vmem=3,
    )(place, tiles, inverse, hats, kept, sent, error)
    return (token_grad, new_error, jnp.swapaxes(hats, 1, 2), jnp.swapaxes(q_new, 1, 2))


def solution(mesh):
    finer = Mesh(mesh.devices.reshape(4, 4, 4, 2), NODE_GRP)
    placed = (
        P(NODE_GRP, None),
        P(NODE_GRP, None),
        P(NODE, None),
        P(NODE, None),
        P(NODE, None),
        P(GRP, NODE, None),
        P(),
    )

    return jax.shard_map(
        on_device,
        mesh=finer,
        in_specs=placed,
        out_specs=(P(NODE_GRP, None), P(GRP, NODE, None), P(None, NODE, None), P()),
        check_vma=False,
    )
```

```python
import functools
import math

import jax
import jax.numpy as jnp
from jax import lax
from jax.experimental import pallas as pl
from jax.experimental.pallas import tpu as pltpu
from jax.sharding import Mesh
from jax.sharding import PartitionSpec as P

Y, X, Z, C = "node_0", "node_1", "grp_0", "grp_1"
NODE = (Y, X)
GRP = (Z, C)
NODE_GRP = (Y, X, Z, C)
BF = jnp.bfloat16
F32 = jnp.float32
HIGH = lax.Precision.HIGHEST


def neighbour(value, stage, by):
    pairs = []
    for device in range(128):
        y, x, z, c = device // 32, device // 8 % 4, device // 2 % 4, device % 2
        if (c == 0) == (stage == 0):
            to = (y, (x + by) % 4, z, c)
        else:
            to = ((y + by) % 4, x, z, c)
        pairs.append((device, to[0] * 32 + to[1] * 8 + to[2] * 2 + to[3]))
    return lax.ppermute(value, NODE_GRP, pairs)


def other_core(value):
    return lax.ppermute(value, C, [(0, 1), (1, 0)])


def exchange(tiles, axis):
    return lax.all_to_all(tiles, axis, split_axis=0, concat_axis=0, tiled=True)


def dot(a, b, ca=1, cb=0, precision=None):
    return lax.dot_general(
        a, b, (((ca,), (cb,)), ((), ())), precision=precision, preferred_element_type=F32
    )


def call(body, out, grid=None, ins=None, outs=None, flops=0, scratch=(), vmem=24):
    params = {}
    if grid is not None:
        params.update(grid=grid, in_specs=ins, out_specs=outs)
    elif ins is not None:
        params.update(in_specs=ins)
    if flops:
        params["cost_estimate"] = pl.CostEstimate(
            flops=flops, bytes_accessed=1 << 20, transcendentals=0
        )
    return pl.pallas_call(
        body,
        out_shape=out,
        scratch_shapes=scratch,
        compiler_params=pltpu.CompilerParams(vmem_limit_bytes=(vmem + vmem // 2 + 6) << 20),
        **params,
    )


SCALAR = pl.BlockSpec(memory_space=pltpu.SMEM)
WHOLE = pl.BlockSpec(memory_space=pltpu.VMEM)


def struct(shape, kind=BF):
    return jax.ShapeDtypeStruct(shape, kind)


def near_struct(shape, kind=BF):
    return pltpu.VMEM(shape, kind)


def far_struct(shape, kind=BF):
    return pltpu.HBM(shape, kind)


def far(*values):
    return tuple(pltpu.with_memory_space_constraint(v, pltpu.HBM) for v in values)


def near(*values):
    return tuple(pltpu.with_memory_space_constraint(v, pltpu.VMEM) for v in values)


def gelu_parts(value):
    coeff = math.sqrt(2.0 / math.pi)
    inner = coeff * (value + 0.044715 * value * value * value)
    tanh_value = jnp.tanh(inner)
    activation = 0.5 * value * (1.0 + tanh_value)
    slope = 0.5 * (1.0 + tanh_value) + 0.5 * value * (1.0 - tanh_value * tanh_value) * coeff * (
        1.0 + 3.0 * 0.044715 * value * value
    )
    return (activation, slope)


def start_body(place_ref, gate_ref, up_ref, down_ref, own_ref):
    half = gate_ref.shape[1] // 2
    core = place_ref[16]
    for m, ref in enumerate((gate_ref, up_ref, down_ref)):
        own_ref[:, m * half : (m + 1) * half] = ref[:, pl.ds(pl.multiple_of(core * half, 128), half)]


def error_body(place_ref, e_ref, mine_ref, send_ref):
    half = mine_ref.shape[1] // 3
    units = 2 * half
    core = place_ref[16]
    for m in range(3):
        at = m * units + core * half
        mine_ref[:, m * half : (m + 1) * half] = e_ref[:, pl.ds(pl.multiple_of(at, 128), half)]
        at = m * units + (1 - core) * half
        send_ref[:, m * half : (m + 1) * half] = e_ref[:, pl.ds(pl.multiple_of(at, 128), half)]


def low_body(own_ref, left_ref, right_ref, low_ref, far_low_ref, far_high_ref):
    rows, at = own_ref.shape[0], far_low_ref.shape[0]
    low_ref[:rows] = own_ref[...]
    low_ref[rows:] = right_ref[...]
    far_low_ref[...] = left_ref[:at]
    far_high_ref[...] = right_ref[at:]


def high_body(far_low_ref, far_high_ref, left_ref, high_ref):
    at, rows = far_low_ref.shape[0], left_ref.shape[0]
    high_ref[:at] = far_low_ref[...]
    high_ref[at:rows] = far_high_ref[...]
    high_ref[rows:] = left_ref[...]


def picked(place_ref, width, rows):
    here = lax.broadcasted_iota(jnp.int32, (width, rows), 0) - place_ref[17]
    return jnp.where(here == lax.broadcasted_iota(jnp.int32, (width, rows), 1), 1.0, 0.0).astype(BF)


def roll_body(order_ref, own_ref, other_ref, out_ref, both_ref, scratch):
    tok, rows = own_ref.shape[0], out_ref.shape[1]
    both_ref[:tok] = own_ref[...]
    both_ref[tok:] = other_ref[...]
    scratch[:, :tok] = own_ref[...].T
    scratch[:, tok:] = other_ref[...].T
    for s in range(out_ref.shape[0]):
        out_ref[s] = scratch[pl.ds(pl.multiple_of(order_ref[s] * rows, 16), rows), :]


def rolled(order, own, other, rows):
    tok, width = own.shape
    roll, both = call(
        roll_body,
        (near_struct((width // rows, rows, 2 * tok)), near_struct((2 * tok, width))),
        ins=[SCALAR, WHOLE, WHOLE],
        scratch=[pltpu.VMEM((width, 2 * tok), BF)],
        vmem=5,
    )(order, own, other)
    return roll, both


def pair(ref, a, b, tok):
    at = pl.multiple_of(pl.program_id(0) * tok, 128)
    value = ref[4 * a + 2 * b : 4 * a + 2 * b + 2, :, pl.ds(at, tok)]
    return value.reshape(-1, tok)


def line(ref, b, tok):
    at = pl.multiple_of(pl.program_id(0) * tok, 128)
    return jnp.concatenate([ref[4 * a + b, :, pl.ds(at, tok)] for a in range(4)], axis=0)


def joined(ref):
    return ref[...].reshape(-1, ref.shape[-1])


def tokens_of(ref, tok):
    return ref.at[pl.ds(pl.multiple_of(pl.program_id(0) * tok, 128), tok), :]


def ahead_body(slots, t_ref, c_ref, *refs):
    tok = t_ref.shape[2] // 2
    out_ref = tokens_of(refs[-1], tok)
    units = out_ref.shape[-1] // 3
    gate_up, back = 0.0, 0.0
    if len(refs) > len(slots) + 1:
        part = tokens_of(refs[-2], tok)
        gate_up, back = part[:, : 2 * units], part[:, 2 * units :]
    for (a, b), piece in zip(slots, refs):
        gate_up = gate_up + dot(pair(t_ref, a, b, tok), piece[:, : 2 * units], 0, 0)
        back = back + dot(pair(c_ref, a, b, tok), piece[:, 2 * units :], 0, 0)
    out_ref[:, : 2 * units] = gate_up
    out_ref[:, 2 * units :] = back


def ahead(slots, t_roll, c_roll, pieces, partial=None):
    both, wide = t_roll.shape[2], pieces[0].shape[1]
    more = () if partial is None else near(partial)
    return call(
        functools.partial(ahead_body, slots),
        near_struct((both, wide), F32),
        grid=(2,),
        ins=[WHOLE] * (2 + len(pieces) + len(more)),
        outs=WHOLE,
        flops=2 * both * wide * pieces[0].shape[0] * len(pieces),
        vmem=5,
    )(*near(t_roll, c_roll), *pieces, *more)


def weight_part(t, c, grads):
    units = grads.shape[1] // 3
    return jnp.concatenate([dot(t, grads[:, : 2 * units]), dot(c, grads[:, 2 * units :])], axis=1)


def late_body(
    scale, groups, place_ref, part_all, t_ref, c_ref, low, high, q_ref, t_both, c_both,
    e_ref, e_other_ref, grads_all, far_own, far_other, power_ref, total, grads_out, far_out, sems
):
    tok = t_ref.shape[2] // 2
    here = pl.program_id(0)
    part_ref = tokens_of(part_all, tok)
    units = part_ref.shape[-1] // 3
    gate_up, back = part_ref[:, : 2 * units], part_ref[:, 2 * units :]
    for b, piece in enumerate((low, high)):
        gate_up = gate_up + dot(pair(t_ref, 2, b, tok), piece[:, : 2 * units], 0, 0)
        back = back + dot(pair(c_ref, 2, b, tok), piece[:, 2 * units :], 0, 0)
    up_pre = gate_up[:, units:]
    activation, slope = gelu_parts(gate_up[:, :units])
    parts = (back * up_pre * slope, back * activation, activation * up_pre)
    parts = [part.astype(BF) for part in parts]
    grads = jnp.concatenate(parts, axis=1)
    grads_out[here] = grads
    far_out[here] = weight_part(line(t_ref, 2, tok), line(c_ref, 2, tok), grads).astype(BF)

    def copies(k):
        rows = grads_all.at[pl.ds(k * tok, tok)]
        return (
            pltpu.make_async_copy(grads_out.at[k], rows, sems.at[2 * k]),
            pltpu.make_async_copy(far_out.at[k], (far_own, far_other)[k], sems.at[2 * k + 1]),
        )

    for k in range(2):

        def leave(k=k):
            for copy in copies(k):
                copy.start()

        pl.when(here == k)(leave)
    first = jnp.concatenate([dot(q_ref[m], parts[m], 1, 1) for m in range(2)], axis=0).astype(BF)
    second = dot(q_ref[2], parts[2], 1, 1).astype(BF)
    split = first.shape[0]
    top, bottom = dot(first, tokens_of(t_both, tok)[...]), dot(second, tokens_of(c_both, tok)[...])

    def start():
        total[:split], total[split:] = top, bottom

    def finish():
        value = jnp.concatenate([top + total[:split], bottom + total[split:]], axis=0)
        width, rows = value.shape[1], e_ref.shape[0]
        error = e_ref[...].astype(F32) + e_other_ref[...].astype(F32)
        error = jnp.concatenate(
            [dot(q_ref[m].astype(F32), error[:, m * units : (m + 1) * units], 1, 1) for m in range(3)],
            axis=0,
        )
        error_high = error.astype(BF)
        error_low = (error - error_high.astype(F32)).astype(BF)
        pick = picked(place_ref, width, rows)
        placed = dot(error_high, pick, 1, 1) + dot(error_low, pick, 1, 1)
        value = (value * scale + placed) * (1.0 / groups)
        step = width // groups
        for i in range(groups):
            power_ref[i] = value[:, i * step : (i + 1) * step].astype(BF)
        for copy in (*copies(0), *copies(1)):
            copy.wait()

    pl.when(pl.program_id(0) == 0)(start)
    pl.when(pl.program_id(0) == 1)(finish)


def near_body(t_one, c_one, t_three, c_three, grads_ref, *outs):
    one = weight_part(joined(t_one), joined(c_one), grads_ref).astype(BF)
    three = weight_part(joined(t_three), joined(c_three), grads_ref).astype(BF)
    for k in range(2):

        def put(k=k):
            outs[k][...] = one
            outs[2 + k][...] = three

        pl.when(pl.program_id(0) == k)(put)


def home_body(t_ref, c_ref, grads_ref, right_own, right_other, left_own, left_other, *outs):
    value = weight_part(joined(t_ref), joined(c_ref), grads_ref)
    rows = outs[0].shape[0]

    def put(k, a, b):
        total = (value + a[...].astype(F32) + b[...].astype(F32)).astype(BF)
        for i in range(4):
            outs[4 * k + i][...] = total[i * rows : (i + 1) * rows]

    pl.when(pl.program_id(0) == 0)(lambda: put(0, right_own, left_own))
    pl.when(pl.program_id(0) == 1)(lambda: put(1, right_other, left_other))


def spread_body(in_ref, out_ref):
    total = in_ref[0].astype(F32)
    for i in range(1, in_ref.shape[0]):
        total = total + in_ref[i].astype(F32)
    total = total.astype(BF)
    for i in range(out_ref.shape[0]):
        out_ref[i] = total


def spread(tiles, count):
    return call(spread_body, far_struct((count, *tiles.shape[1:])), vmem=4)(tiles)


def joined_lanes(p_ref):
    return jnp.concatenate([p_ref[i].astype(F32) for i in range(p_ref.shape[0])], axis=1).astype(BF)


def right_body(
    scale, groups, place_ref, p_ref, t_ref, c_ref, y_ref, e_ref, e_other_ref, out_ref, total
):
    power = joined_lanes(p_ref)
    rank = power.shape[0] // 3
    units = y_ref.shape[1] // 3
    seen = dot(power[: 2 * rank], t_ref[...], 1, 1).astype(BF)
    lhs = (seen[:rank], seen[rank:], dot(power[2 * rank :], c_ref[...], 1, 1).astype(BF))
    values = [dot(lhs[m], y_ref[:, m * units : (m + 1) * units]) for m in range(3)]

    def start():
        for m in range(3):
            total[m] = values[m]

    def finish():
        rows = dot(power, picked(place_ref, power.shape[1], e_ref.shape[0])).astype(BF)
        error = (e_ref[...].astype(F32) + e_other_ref[...].astype(F32)).astype(BF)
        for m in range(3):
            value = (values[m] + total[m]) * scale
            value = value + dot(
                rows[m * rank : (m + 1) * rank], error[:, m * units : (m + 1) * units]
            )
            value = (value * (1.0 / groups)).astype(BF)
            step = units // 4
            for i in range(4):
                out_ref[i, m * rank : (m + 1) * rank] = value[:, i * step : (i + 1) * step]

    pl.when(pl.program_id(0) == 0)(start)
    pl.when(pl.program_id(0) == 1)(finish)


def factor_body(place_ref, p_ref, inverse_ref, hats_ref):
    low = joined_lanes(p_ref)
    r = low.shape[0] // 3
    gram = jnp.stack(
        [dot(low[m * r : (m + 1) * r], low[m * r : (m + 1) * r], 1, 1) for m in range(3)]
    )
    rows = lax.broadcasted_iota(jnp.int32, (3, r, 2 * r), 1)
    cols = lax.broadcasted_iota(jnp.int32, (3, r, 2 * r), 2)
    both = jnp.concatenate([gram, jnp.zeros((3, r, r), F32)], axis=2)
    both = both + jnp.where(cols == rows + r, 1.0, 0.0)
    for j in range(r):
        column = jnp.where(rows[:, :, :1] > j, both[:, :, j : j + 1], 0.0)
        row = both[:, j : j + 1, :] / both[:, j : j + 1, j : j + 1]
        both = both - column * row
    diagonal = jnp.sum(jnp.where(cols == rows, both, 0.0), axis=2, keepdims=True)
    inverse = both[:, :, r:] * (1.0 / jnp.sqrt(diagonal))
    inverse_ref[...] = inverse
    mine = dot(low, picked(place_ref, low.shape[1], hats_ref.shape[2]))
    for m in range(3):
        hats_ref[m] = dot(inverse[m], mine[m * r : (m + 1) * r], 1, 0, HIGH)


def final_body(scale, core_ref, b_ref, inverse_ref, hats_ref, kept_ref, sent_ref, e_ref, err_ref, q_ref):
    r = inverse_ref.shape[1]
    units = q_ref.shape[2]
    half = units // 2
    core = core_ref[16]
    for m in range(3):
        right = jnp.concatenate(
            [b_ref[i, m * r : (m + 1) * r].astype(F32) for i in range(b_ref.shape[0])], axis=1
        )
        q_t = dot(inverse_ref[m], right, 1, 0, HIGH)
        q_ref[m] = q_t
        rebuilt = dot(hats_ref[m].astype(BF), q_t.astype(BF), 0, 0)
        kept = kept_ref[:, m * half : (m + 1) * half].astype(F32)
        sent = sent_ref[:, m * half : (m + 1) * half].astype(F32)
        for side in range(2):
            at = slice(m * units + side * half, m * units + (side + 1) * half)
            grad = jnp.where(core == side, kept, sent)
            value = grad * scale + e_ref[:, at].astype(F32)
            err_ref[0, :, at] = (value - rebuilt[:, side * half : (side + 1) * half]).astype(BF)


def token_body(order_ref, y_ref, *refs):
    own_ref, other_ref = refs[-2:]
    rows, tok = own_ref.shape[1:]
    wide = y_ref.shape[1] // 3 * 2
    for s in range(0, own_ref.shape[0], 2):
        value = dot(refs[s // 2][:, :wide], y_ref[:, :wide], 1, 1).astype(BF)
        for i in range(2):
            at = order_ref[s + i]
            own_ref[at] = value[i * rows : (i + 1) * rows, :tok]
            other_ref[at] = value[i * rows : (i + 1) * rows, tok:]


def turn_body(a_ref, b_ref, out_ref):
    value = a_ref[...].astype(F32) + b_ref[...].astype(F32)
    out_ref[...] = value.T.astype(BF)


def on_device(tokens, cotangent, gate_weight, up_weight, down_weight_t, error_memory, q_init):
    yi, xi, core = lax.axis_index(Y), lax.axis_index(X), lax.axis_index(C)
    rows, units = gate_weight.shape
    node_count, groups = lax.axis_size(NODE), lax.axis_size(GRP)
    half, rank = units // 2, q_init.shape[-1]
    tok, width = tokens.shape
    grad_scale = 1.0 / math.sqrt(tok * node_count)

    def first(value, by):
        return neighbour(value, 0, by)

    def second(value, by):
        return neighbour(value, 1, by)

    over, along = jnp.arange(4)[:, None], jnp.arange(4)[None, :]
    ys = jnp.where(core == 0, yi + over, yi + along) % 4
    xs = jnp.where(core == 0, xi + along, xi + over) % 4
    place = jnp.concatenate(
        [(ys * 4 + xs).reshape(-1), core.reshape(1), ((yi * 4 + xi) * rows).reshape(1)]
    ).astype(jnp.int32)

    wide = 3 * half
    error = error_memory[0]
    weights = [
        pltpu.with_memory_space_constraint(w, pltpu.HBM)
        for w in (gate_weight, up_weight, down_weight_t)
    ]
    own = call(start_body, struct((rows, wide)), ins=[SCALAR] + [WHOLE] * 3, vmem=3)(place, *weights)
    from_left, from_right = first(own, 1), first(own, -1)
    other_t, other_c = other_core(tokens), other_core(cotangent)
    e_mine, e_send = call(
        error_body, (struct((rows, wide)),) * 2, ins=[SCALAR, WHOLE], vmem=3
    )(place, error)
    e_other = other_core(e_send)
    t_roll, t_both = rolled(place, tokens, other_t, rows)
    from_left, from_right, t_roll = lax.optimization_barrier((from_left, from_right, t_roll))
    at = rows // 32 * 16
    low, far_low, far_high = call(
        low_body,
        (struct((2 * rows, wide)), struct((at, wide)), struct((rows - at, wide))),
        vmem=2,
    )(own, from_left, from_right)
    far_low = first(far_low, 1)
    far_high = first(far_high, -1)
    left_low = second(low, 1)
    right_low = second(low, -1)
    c_roll, c_both = rolled(place, cotangent, other_c, rows)
    high = call(high_body, struct((2 * rows, wide)), vmem=2)(far_low, far_high, from_left)
    left_high = second(high, 1)
    right_high = second(high, -1)
    over_low, over_high = second(left_low, 1), second(right_high, -1)
    q_rows = lax.dynamic_slice_in_dim(jnp.swapaxes(q_init, 1, 2), core * half, half, 2).astype(BF)

    slots = ((0, 0), (0, 1), (3, 0), (1, 0))
    partial = ahead(slots, t_roll, c_roll, (low, high, left_low, right_low))
    partial = ahead(((3, 1), (1, 1)), t_roll, c_roll, (left_high, right_high), partial)
    long, mine = (4 * rows, wide), (groups, 3 * rank, width // groups)
    block = pl.BlockSpec((tok, wide), lambda k: (k, 0))

    def slot(b):
        return pl.BlockSpec((4, 1, rows, tok), lambda k: (0, b, 0, k))

    def fixed(*shape):
        return pl.BlockSpec(shape, lambda k: (0,) * len(shape))

    grads, far_own, far_other, power = call(
        functools.partial(late_body, grad_scale, groups),
        (far_struct((2 * tok, wide)), far_struct(long), far_struct(long), far_struct(mine)),
        grid=(2,),
        ins=[SCALAR] + [WHOLE] * 10,
        outs=(pl.BlockSpec(memory_space=pltpu.HBM),) * 3 + (fixed(*mine),),
        scratch=[
            pltpu.VMEM((3 * rank, width), F32),
            pltpu.VMEM((2, tok, wide), BF),
            pltpu.VMEM((2, *long), BF),
            pltpu.SemaphoreType.DMA((4,)),
        ],
        flops=2 * 2 * tok * 8 * rows * wide,
        vmem=16,
    )(
        place, *near(partial, t_roll, c_roll), over_low, over_high, q_rows, *near(t_both, c_both),
        e_mine, e_other,
    )

    four = (4, 4, rows, 2 * tok)
    rolls = far(t_roll.reshape(four), c_roll.reshape(four))
    one_own, one_other, three_own, three_other = call(
        near_body,
        (far_struct(long),) * 4,
        grid=(2,),
        ins=[slot(1), slot(1), slot(3), slot(3), block],
        outs=(fixed(*long),) * 4,
        flops=2 * 2 * tok * 8 * rows * wide,
        vmem=16,
    )(*rolls, *rolls, *far(grads))

    power = spread(exchange(power, GRP), node_count)
    power, one_other, three_own = lax.optimization_barrier((power, one_other, three_own))
    power = spread(exchange(power, NODE), groups)
    power = exchange(power, GRP)

    def relay(send, away_own, away_other, one_own, one_other, three_own, three_other):
        to_right, to_left = send(away_own, 1), send(away_other, -1)
        left_other, right_own = send(one_other, 1), send(three_own, -1)
        left_own = send((one_own.astype(F32) + to_right.astype(F32)).astype(BF), 1)
        right_other = send((three_other.astype(F32) + to_left.astype(F32)).astype(BF), -1)
        return right_own, right_other, left_own, left_other

    terms = relay(first, far_own, far_other, one_own, one_other, three_own, three_other)
    sums = call(
        home_body,
        (far_struct((rows, wide)),) * 8,
        grid=(2,),
        ins=[slot(0), slot(0), block] + [fixed(*long)] * 4,
        outs=(fixed(rows, wide),) * 8,
        flops=2 * 2 * tok * 4 * rows * wide,
        vmem=16,
    )(*rolls, *far(grads), *far(*terms))
    own_sums, other_sums = sums[:4], sums[4:]
    right_own, right_other, left_own, left_other = relay(
        second, own_sums[2], other_sums[2], own_sums[1], other_sums[1], own_sums[3], other_sums[3]
    )

    def total(value, a, b):
        return (value.astype(F32) + a.astype(F32) + b.astype(F32)).astype(BF)

    kept = total(own_sums[0], right_own, left_own)
    sent = other_core(total(other_sums[0], right_other, left_other))

    tiles = call(
        functools.partial(right_body, grad_scale, groups),
        far_struct((4, 3 * rank, half // 4)),
        grid=(2,),
        ins=[SCALAR, WHOLE] + [pl.BlockSpec((tok, width), lambda k: (k, 0))] * 2 + [block] + [fixed(rows, wide)] * 2,
        outs=fixed(4, 3 * rank, half // 4),
        scratch=[pltpu.VMEM((3, rank, half), F32)],
        flops=4 * 3 * rank * 2 * tok * width,
        vmem=12,
    )(place, power, *far(t_both, c_both, grads, e_mine, e_other))
    tiles = spread(exchange(tiles, Z), node_count)
    tiles = spread(exchange(tiles, NODE), groups)
    tiles = exchange(tiles, (C, Z))
    inverse, hats = call(
        factor_body,
        (struct((3, rank, rank), F32), struct((3, rank, rows), F32)),
        ins=[SCALAR, WHOLE],
        flops=1 << 24,
        vmem=2,
    )(place, power)

    pieces = (low, high, right_low, right_high, over_low, over_high, left_low, left_high)
    token_own, token_other = call(
        token_body,
        (struct((node_count, rows, tok)),) * 2,
        ins=[SCALAR] + [WHOLE] * 9,
        flops=2 * 2 * tok * width * 2 * half,
        vmem=12,
    )(place, *far(grads, *pieces))
    token_grad = call(turn_body, struct((tok, width)), vmem=4)(
        token_own.reshape(width, tok), other_core(token_other).reshape(width, tok)
    )

    new_error, q_new = call(
        functools.partial(final_body, grad_scale),
        (struct((1, rows, 3 * units)), struct((3, rank, units), F32)),
        ins=[SCALAR] + [WHOLE] * 6,
        vmem=3,
    )(place, tiles, inverse, hats, kept, sent, error)
    return (token_grad, new_error, jnp.swapaxes(hats, 1, 2), jnp.swapaxes(q_new, 1, 2))


def solution(mesh):
    finer = Mesh(mesh.devices.reshape(4, 4, 4, 2), NODE_GRP)
    placed = (
        P(NODE_GRP, None),
        P(NODE_GRP, None),
        P(NODE, None),
        P(NODE, None),
        P(NODE, None),
        P(GRP, NODE, None),
        P(),
    )

    return jax.shard_map(
        on_device,
        mesh=finer,
        in_specs=placed,
        out_specs=(P(NODE_GRP, None), P(GRP, NODE, None), P(None, NODE, None), P()),
        check_vma=False,
    )
```
